256 devices in a mesh: ka: 32 (over z, x_lo, core), sp: 8 (over y, x_hi).
Axes of the slice: x: 4 (x_hi: 2, x_lo: 2; x = x_hi * 2 + x_lo), y: 4, z: 8, core: 2. Of those that a mesh axis runs over, the one named last changes fastest.
Arguments:
- bloch_index: int32 [32, 2], P('ka'), may hold values from 0 to 63
- material: int32 [128, 64, 128], P('sp'), may hold values from 0 to 2
- permittivity: float32 [3], replicated, may hold values from 1 to 12
- absorption_peak: float32 [1], replicated, may hold values from 0.25 to 2
- source_sheet: float32 [32, 2, 128, 64], P('ka', None, 'sp'), may hold values from -6 to 6
- waveform: float32 [10], replicated, may hold values from -6 to 6
- electric_in: bfloat16 [32, 6, 128, 64, 128], P('ka', None, 'sp'), may hold values from -12 to 12
- magnetic_in: bfloat16 [32, 6, 128, 64, 128], P('ka', None, 'sp'), may hold values from -12 to 12
Outputs:
- electric_out: float32 [32, 6, 128, 64, 128], P('ka', None, 'sp')
- magnetic_out: float32 [32, 6, 128, 64, 128], P('ka', None, 'sp')
- reflected: float32 [32, 2], P('ka')
- reflected_mean: float32 [2], replicated
The draws below stay inside these ranges and needn't reach their ends.
All inputs are finite; a program needn't handle non-finite values.
Results may differ from the reference program's by a relative error of at most 0.0003.
Values sent between devices are 32-bit elements; how exact they have to be, the bound alone decides.
A program may use at most 64 MiB of HBM per device.

```python
import math
import jax
import jax.numpy as jnp
from jax import lax

NY = 64
NZ = 128
PML = 16
STEPS = 10
INTERVAL = 5
NSNAP = 2
MPHASE = 64
NMAT = 3
K = 32
NX = 128


def start_field(key, salt):
    key = jax.random.fold_in(key, salt)
    level_key, phase_key, noise_key, common_key = jax.random.split(key, 4)
    level = jax.random.uniform(level_key, (K, 1, 1, 1, 1), jnp.float32, -1.0, 1.0)
    amplitude = jnp.exp(0.6931472 * level)
    phase = jax.random.uniform(phase_key, (K, 1, 1, 1, 1), jnp.float32, 0.0, 6.2831853)
    across = jnp.arange(NX, dtype=jnp.float32).reshape(1, 1, NX, 1, 1)
    profile = 1.0 + 0.6 * jnp.sin(6.2831853 * across / NX + phase)
    full_shape = (K, 6, NX, NY, NZ)
    rough = jnp.clip(jax.random.normal(noise_key, full_shape, jnp.float32), -3.5, 3.5)
    return (amplitude * profile * rough).astype(jnp.bfloat16)


def draw_electric_in(key, part):
    return start_field(key, 11)


def draw_magnetic_in(key, part):
    return start_field(key, 23)


def set_ends(values, rng, low, top_value):
    longest = values.shape.index(max(values.shape))
    spots = []
    for shift in (0, 1):
        where = [jax.random.randint(jax.random.fold_in(rng, axis), (), 0, length) for axis, length in enumerate(values.shape)]
        where[longest] = (where[longest] + shift) % values.shape[longest]
        spots.append(tuple(where))
    return values.at[spots[0]].set(low).at[spots[1]].set(top_value)


def block_scale(rng, dims, cuts, low, largest):
    gain = 1.0
    for position, blocks in cuts:
        heights = jax.random.uniform(jax.random.fold_in(jax.random.fold_in(rng, 6), position), (blocks,), jnp.float32, low / len(cuts), largest / len(cuts))
        gain = gain * jnp.repeat(jnp.exp(heights), dims[position] // blocks).reshape((-1,) + (1,) * (len(dims) - 1 - position))
    return gain


def normal_values(stream_key, extent, deviation, reach, shards=(), kind=jnp.bfloat16):
    values = deviation * jax.random.normal(stream_key, extent, jnp.float32)
    if shards:
        values = values * block_scale(stream_key, extent, shards, -0.22, 0.18)
    return jnp.clip(values, -reach, reach).astype(kind)


def setup_inputs(seed: int = 0) -> dict:
    keys = jax.random.split(jax.random.key(seed), 9)
    bloch_index = set_ends(jax.random.randint(keys[0], (K, 2), 0, MPHASE), jax.random.fold_in(keys[0], 1), 0, MPHASE - 1).astype(jnp.int32)
    material = set_ends(jax.random.randint(keys[1], (NX, NY, NZ), 0, NMAT), jax.random.fold_in(keys[1], 1), 0, NMAT - 1).astype(jnp.int32)
    permittivity = jnp.clip(jnp.exp(jax.random.uniform(keys[2], (NMAT,), jnp.float32, math.log(1.0), math.log(12.0))), 1.0, 12.0)
    absorption_peak = jnp.clip(jnp.exp(jax.random.uniform(keys[3], (1,), jnp.float32, math.log(0.25), math.log(2.0))), 0.25, 2.0)
    source_sheet = normal_values(keys[4], (K, 2, NX, NY), 1.0, 6.0, ((0, 32), (2, 8)), jnp.float32)
    waveform = normal_values(keys[5], (STEPS,), 1.0, 6.0, (), jnp.float32)
    electric_in = draw_electric_in(jax.random.fold_in(keys[8], 71), 0)
    magnetic_in = draw_magnetic_in(jax.random.fold_in(keys[8], 71), 0)
    return dict(bloch_index=bloch_index, material=material, permittivity=permittivity, absorption_peak=absorption_peak, source_sheet=source_sheet, waveform=waveform, electric_in=electric_in, magnetic_in=magnetic_in)


TIME_STEP = 0.5


def rotate(couple, cosine, sine):
    return (couple[0] * cosine - couple[1] * sine, couple[0] * sine + couple[1] * cosine)


def subtract(left, right):
    return (left[0] - right[0], left[1] - right[1])


def slice_along(couple, begin_at, end_at, along):
    return tuple(lax.slice_in_dim(values, begin_at, end_at, axis=along) for values in couple)


def attach(front, back, along):
    return tuple(jnp.concatenate([first_part, second_part], axis=along) for first_part, second_part in zip(front, back))


def above_cell(couple, beyond, along):
    length = couple[0].shape[along]
    return attach(slice_along(couple, 1, length, along), beyond, along)


def below_cell(couple, beyond, along):
    length = couple[0].shape[along]
    return attach(beyond, slice_along(couple, 0, length - 1, along), along)


def forward_wrap(couple, along, cosine, sine):
    beyond = rotate(slice_along(couple, 0, 1, along), cosine, sine)
    return subtract(above_cell(couple, beyond, along), couple)


def backward_wrap(couple, along, cosine, sine):
    length = couple[0].shape[along]
    beyond = rotate(slice_along(couple, length - 1, length, along), cosine, -sine)
    return subtract(couple, below_cell(couple, beyond, along))


def forward_open(couple):
    along = couple[0].ndim - 1
    beyond = tuple(jnp.zeros_like(values) for values in slice_along(couple, 0, 1, along))
    return subtract(above_cell(couple, beyond, along), couple)


def backward_open(couple):
    along = couple[0].ndim - 1
    beyond = tuple(jnp.zeros_like(values) for values in slice_along(couple, 0, 1, along))
    return subtract(couple, below_cell(couple, beyond, along))


def electric_curl(electric, beyond_y, beyond_z, cosine, sine):
    ex_part, ey_part, ez_part = electric
    across = ex_part[0].ndim - 3
    sideways = across + 1
    dx_ey = subtract(above_cell(ey_part, beyond_y, across), ey_part)
    dx_ez = subtract(above_cell(ez_part, beyond_z, across), ez_part)
    return (subtract(forward_wrap(ez_part, sideways, cosine, sine), forward_open(ey_part)),
            subtract(forward_open(ex_part), dx_ez),
            subtract(dx_ey, forward_wrap(ex_part, sideways, cosine, sine)))


def magnetic_curl(magnetic, behind_y, behind_z, cosine, sine):
    hx_part, hy_part, hz_part = magnetic
    across = hx_part[0].ndim - 3
    sideways = across + 1
    bx_hy = subtract(hy_part, below_cell(hy_part, behind_y, across))
    bx_hz = subtract(hz_part, below_cell(hz_part, behind_z, across))
    return (subtract(backward_wrap(hz_part, sideways, cosine, sine), backward_open(hy_part)),
            subtract(backward_open(hx_part), bx_hz),
            subtract(bx_hy, backward_wrap(hx_part, sideways, cosine, sine)))


def relax(couple, change, retain, factor):
    return (retain * couple[0] + factor * change[0], retain * couple[1] + factor * change[1])


def coefficients(material, permittivity, absorption_peak, depth):
    height = jnp.arange(depth, dtype=jnp.float32)
    low_depth = jnp.maximum(PML - height, 0.0) / PML
    high_depth = jnp.maximum(height - (depth - 1 - PML), 0.0) / PML
    conduct = absorption_peak[0] * (low_depth ** 3 + high_depth ** 3)
    half_mag = conduct * (0.5 * TIME_STEP)
    h_retain = (1.0 - half_mag) / (1.0 + half_mag)
    h_factor = -TIME_STEP / (1.0 + half_mag)
    relative = jnp.zeros(material.shape, jnp.float32)
    for level in range(NMAT):
        relative = relative + jnp.where(material == level, permittivity[level], 0.0)
    half_ele = conduct * (0.5 * TIME_STEP) / relative
    e_retain = (1.0 - half_ele) / (1.0 + half_ele)
    e_factor = TIME_STEP / relative / (1.0 + half_ele)
    return e_retain, e_factor, h_retain, h_factor


def reference(bloch_index, material, permittivity, absorption_peak, source_sheet, waveform, electric_in, magnetic_in):
    depth = material.shape[2]
    rows = material.shape[0]
    e_retain, e_factor, h_retain, h_factor = coefficients(material, permittivity, absorption_peak, depth)
    plane = (jnp.arange(depth) == PML + 2).astype(jnp.float32)
    monitor = PML + 6
    angles = 2.0 * jnp.pi * bloch_index.astype(jnp.float32) / MPHASE

    def one_point(inputs):
        angle_pair, sheet_pair, electric_begin, magnetic_begin = inputs
        cos_x = jnp.cos(angle_pair[0])
        sin_x = jnp.sin(angle_pair[0])
        cos_y = jnp.cos(angle_pair[1])
        sin_y = jnp.sin(angle_pair[1])
        sheet = (sheet_pair[0][:, :, None] * plane, sheet_pair[1][:, :, None] * plane)

        def advance(fields, drive):
            electric, magnetic = fields
            beyond_y = rotate(slice_along(electric[1], 0, 1, 0), cos_x, sin_x)
            beyond_z = rotate(slice_along(electric[2], 0, 1, 0), cos_x, sin_x)
            change = electric_curl(electric, beyond_y, beyond_z, cos_y, sin_y)
            magnetic = tuple(relax(couple, change_part, h_retain, h_factor) for couple, change_part in zip(magnetic, change))
            behind_y = rotate(slice_along(magnetic[1], rows - 1, rows, 0), cos_x, -sin_x)
            behind_z = rotate(slice_along(magnetic[2], rows - 1, rows, 0), cos_x, -sin_x)
            change = magnetic_curl(magnetic, behind_y, behind_z, cos_y, sin_y)
            first_change = (change[0][0] - drive * sheet[0], change[0][1] - drive * sheet[1])
            change = (first_change, change[1], change[2])
            electric = tuple(relax(couple, change_part, e_retain, e_factor) for couple, change_part in zip(electric, change))
            return (electric, magnetic)

        def snapshot(fields, index):
            fields = lax.fori_loop(0, INTERVAL, lambda inner, held: advance(held, waveform[index * INTERVAL + inner]), fields)
            electric = fields[0]
            power = (electric[0][0][:, :, monitor] ** 2 + electric[0][1][:, :, monitor] ** 2
                     + electric[1][0][:, :, monitor] ** 2 + electric[1][1][:, :, monitor] ** 2)
            return fields, jnp.sum(power) / power.size

        electric_wide = electric_begin.astype(jnp.float32)
        magnetic_wide = magnetic_begin.astype(jnp.float32)
        start_e = tuple((electric_wide[2 * member], electric_wide[2 * member + 1]) for member in range(3))
        start_h = tuple((magnetic_wide[2 * member], magnetic_wide[2 * member + 1]) for member in range(3))
        final, powers = lax.scan(snapshot, (start_e, start_h), jnp.arange(NSNAP))
        electric, magnetic = final
        electric_stack = jnp.stack([values for couple in electric for values in couple], 0)
        magnetic_stack = jnp.stack([values for couple in magnetic for values in couple], 0)
        return electric_stack, magnetic_stack, powers

    electric_out, magnetic_out, reflected = lax.map(one_point, (angles, source_sheet, electric_in, magnetic_in))
    reflected_mean = jnp.sum(reflected, 0) / reflected.shape[0]
    return electric_out, magnetic_out, reflected, reflected_mean
```

```python
import functools

import jax
import jax.numpy as jnp
from jax import lax
from jax.experimental import pallas as pl
from jax.experimental.pallas import tpu as pltpu
from jax.sharding import PartitionSpec as P

PML = 16
INTERVAL = 5
NSNAP = 2
MPHASE = 64
NMAT = 3
TIME_STEP = 0.5

MESH = pl.DeviceIdType.MESH
F32 = jnp.float32
TILE = 8
CHUNK = 8


def sent_to_all(shard, axis):
    copies = jnp.broadcast_to(shard, (lax.axis_size(axis), *shard.shape))
    return lax.all_to_all(copies, axis, split_axis=0, concat_axis=0, tiled=True)


def of_everyone(shard, axis):
    return sent_to_all(shard, axis).sum(axis=0)


def kernel(
    slabs,
    rows,
    width,
    depth,
    trig,
    permittivity,
    absorption_peak,
    waveform,
    sheet_in,
    material,
    e_in,
    h_in,
    e_out,
    h_out,
    power_out,
    ef,
    hf,
    e_low,
    h_low,
    mat,
    keep,
    gain,
    sheet,
    e_from,
    h_from,
    load_sem,
    store_sem,
    e_send,
    e_recv,
    h_send,
    h_recv,
):
    ka = lax.axis_index("ka")
    sp = lax.axis_index("sp")
    up = lax.rem(sp + 1, slabs)
    down = lax.rem(sp + slabs - 1, slabs)
    chunks = width // CHUNK
    tiles = width // TILE
    last = rows - 1
    steps = NSNAP * INTERVAL

    first_load = pltpu.make_async_copy(
        e_in.at[0, pl.ds(2, 4), pl.ds(0, 1)], e_low.at[pl.ds(2, 4), pl.ds(0, 1)], load_sem.at[0]
    )
    loads = [
        first_load,
        pltpu.make_async_copy(
            e_in.at[0, pl.ds(0, 2), pl.ds(0, 1)],
            e_low.at[pl.ds(0, 2), pl.ds(0, 1)],
            load_sem.at[1],
        ),
        pltpu.make_async_copy(
            e_in.at[0, :, pl.ds(1, last)], e_low.at[:, pl.ds(1, last)], load_sem.at[2]
        ),
        pltpu.make_async_copy(h_in.at[0], h_low, load_sem.at[3]),
        pltpu.make_async_copy(material, mat, load_sem.at[4]),
    ]
    for load in loads:
        load.start()

    barrier = pltpu.get_barrier_semaphore()
    for other in (up, down):
        pl.semaphore_signal(barrier, inc=1, device_id=(ka, other), device_id_type=MESH)

    def e_copy(chunk):
        where = pl.ds(pl.multiple_of(chunk * CHUNK, CHUNK), CHUNK)
        return pltpu.make_async_remote_copy(
            src_ref=ef.at[pl.ds(2, 4), 0, where],
            dst_ref=e_from.at[:, where],
            send_sem=e_send.at[chunk],
            recv_sem=e_recv.at[chunk],
            device_id=(ka, down),
            device_id_type=MESH,
        )

    def h_copy(chunk):
        begin = pl.multiple_of(chunk * CHUNK, CHUNK)
        return pltpu.make_async_remote_copy(
            src_ref=hf.at[pl.ds(2, 4), last, pl.ds(begin + TILE, CHUNK)],
            dst_ref=h_from.at[:, pl.ds(begin, CHUNK)],
            send_sem=h_send.at[chunk],
            recv_sem=h_recv.at[chunk],
            device_id=(ka, up),
            device_id_type=MESH,
        )

    cos_x, sin_x, cos_y, sin_y = trig[0], trig[1], trig[2], trig[3]
    at_end = sp == slabs - 1
    at_start = sp == 0
    end_cos = jnp.where(at_end, cos_x, 1.0)
    end_sin = jnp.where(at_end, sin_x, 0.0)
    start_cos = jnp.where(at_start, cos_x, 1.0)
    start_sin = jnp.where(at_start, -sin_x, 0.0)

    lane = lax.broadcasted_iota(jnp.int32, (TILE, depth), 1)
    at_top = lane == depth - 1
    at_bottom = lane == 0

    def z_above(values):
        return jnp.where(at_top, 0.0, pltpu.roll(values, depth - 1, 1))

    def z_below(values):
        return jnp.where(at_bottom, 0.0, pltpu.roll(values, 1, 1))

    height = lane.astype(F32)
    low_depth = jnp.maximum(PML - height, 0.0) / PML
    high_depth = jnp.maximum(height - (depth - 1 - PML), 0.0) / PML
    conduct = absorption_peak[0] * (low_depth**3 + high_depth**3)
    half_mag = conduct * (0.5 * TIME_STEP)
    h_keep = (1.0 - half_mag) / (1.0 + half_mag)
    h_gain = -TIME_STEP / (1.0 + half_mag)

    first_load.wait()
    for part in range(2, 6):
        ef[part, 0, pl.ds(0, width), :] = e_low[part, 0].astype(F32)
    pl.semaphore_wait(barrier, 2)
    for chunk in range(chunks):
        e_copy(chunk).start()

    def fill_e_edge(x):
        for part in (0, 4):
            real = ef[part, x, pl.ds(0, 1), :]
            imag = ef[part + 1, x, pl.ds(0, 1), :]
            ef[part, x, pl.ds(width, 1), :] = real * cos_y - imag * sin_y
            ef[part + 1, x, pl.ds(width, 1), :] = real * sin_y + imag * cos_y

    def fill_h_edge(x):
        for part in (0, 4):
            real = hf[part, x, pl.ds(width + TILE - 1, 1), :]
            imag = hf[part + 1, x, pl.ds(width + TILE - 1, 1), :]
            hf[part, x, pl.ds(TILE - 1, 1), :] = real * cos_y + imag * sin_y
            hf[part + 1, x, pl.ds(TILE - 1, 1), :] = imag * cos_y - real * sin_y

    for load in loads[1:]:
        load.wait()
    for part in range(2):
        ef[part, 0, pl.ds(0, width), :] = e_low[part, 0].astype(F32)

    def widen_e(x, carry):
        for part in range(6):
            ef[part, x, pl.ds(0, width), :] = e_low[part, x].astype(F32)
        fill_e_edge(x)
        return carry

    def widen_h(x, carry):
        for part in range(6):
            hf[part, x, pl.ds(TILE, width), :] = h_low[part, x].astype(F32)
        return carry

    fill_e_edge(0)
    lax.fori_loop(1, rows, widen_e, 0)
    lax.fori_loop(0, rows, widen_h, 0)

    keeps = []
    gains = []
    for level in range(NMAT):
        relative = permittivity[level]
        half_ele = conduct * (0.5 * TIME_STEP) / relative
        keeps.append((1.0 - half_ele) / (1.0 + half_ele))
        gains.append(TIME_STEP / jnp.full((TILE, depth), relative, F32) / (1.0 + half_ele))

    def fill_coefficients(x, carry):
        for tile in range(tiles):
            where = pl.ds(tile * TILE, TILE)
            kind = mat[x, where, :]
            keep[x, where, :] = jnp.where(
                kind == 0, keeps[0], jnp.where(kind == 1, keeps[1], keeps[2])
            )
            gain[x, where, :] = jnp.where(
                kind == 0, gains[0], jnp.where(kind == 1, gains[1], gains[2])
            )
        return carry

    lax.fori_loop(0, rows, fill_coefficients, 0)

    at_sheet = lax.broadcasted_iota(jnp.int32, (width, depth), 1) == PML + 2
    for part in range(2):
        turned = sheet_in[0, part].T
        for x in range(rows):
            spread = jnp.broadcast_to(turned[:, x : x + 1], (width, depth))
            sheet[part, x] = jnp.where(at_sheet, spread, 0.0)

    def h_x(part, x, begin):
        ey = ef[2 + part, x, pl.ds(begin, TILE), :]
        ez = ef[4 + part, x, pl.ds(begin, TILE), :]
        ez_y = ef[4 + part, x, pl.ds(begin + 1, TILE), :]
        change = (ez_y - ez) - (z_above(ey) - ey)
        where = pl.ds(begin + TILE, TILE)
        hf[part, x, where, :] = h_keep * hf[part, x, where, :] + h_gain * change

    def h_yz(part, x, begin, ey_x, ez_x):
        ex = ef[part, x, pl.ds(begin, TILE), :]
        ex_y = ef[part, x, pl.ds(begin + 1, TILE), :]
        ey = ef[2 + part, x, pl.ds(begin, TILE), :]
        ez = ef[4 + part, x, pl.ds(begin, TILE), :]
        where = pl.ds(begin + TILE, TILE)
        change_y = (z_above(ex) - ex) - (ez_x - ez)
        change_z = (ey_x - ey) - (ex_y - ex)
        hf[2 + part, x, where, :] = h_keep * hf[2 + part, x, where, :] + h_gain * change_y
        hf[4 + part, x, where, :] = h_keep * hf[4 + part, x, where, :] + h_gain * change_z

    def e_x(part, x, begin, drive):
        where = pl.ds(begin, TILE)
        hy = hf[2 + part, x, pl.ds(begin + TILE, TILE), :]
        hz = hf[4 + part, x, pl.ds(begin + TILE, TILE), :]
        hz_y = hf[4 + part, x, pl.ds(begin + TILE - 1, TILE), :]
        change = (hz - hz_y) - (hy - z_below(hy)) - drive * sheet[part, x, where, :]
        ef[part, x, where, :] = (
            keep[x, where, :] * ef[part, x, where, :] + gain[x, where, :] * change
        )

    def e_yz(part, x, begin, hy_x, hz_x):
        where = pl.ds(begin, TILE)
        hx = hf[part, x, pl.ds(begin + TILE, TILE), :]
        hx_y = hf[part, x, pl.ds(begin + TILE - 1, TILE), :]
        hy = hf[2 + part, x, pl.ds(begin + TILE, TILE), :]
        hz = hf[4 + part, x, pl.ds(begin + TILE, TILE), :]
        change_y = (hx - z_below(hx)) - (hz - hz_x)
        change_z = (hy - hy_x) - (hx - hx_y)
        retain = keep[x, where, :]
        factor = gain[x, where, :]
        ef[2 + part, x, where, :] = retain * ef[2 + part, x, where, :] + factor * change_y
        ef[4 + part, x, where, :] = retain * ef[4 + part, x, where, :] + factor * change_z

    def turned_pair(source, part, where, cosine, sine):
        real = source[part, where, :]
        imag = source[part + 1, where, :]
        return (real * cosine - imag * sine, real * sine + imag * cosine)

    def h_boundary(chunk, carry):
        e_copy(chunk).wait()
        for tile in range(CHUNK // TILE):
            begin = pl.multiple_of(chunk * CHUNK + tile * TILE, TILE)
            ey_x = turned_pair(e_from, 0, pl.ds(begin, TILE), end_cos, end_sin)
            ez_x = turned_pair(e_from, 2, pl.ds(begin, TILE), end_cos, end_sin)
            for part in range(2):
                h_yz(part, last, begin, ey_x[part], ez_x[part])
        h_copy(chunk).start()
        return carry

    def h_row(x, carry):
        for tile in range(tiles):
            begin = tile * TILE
            where = pl.ds(begin, TILE)
            for part in range(2):
                h_x(part, x, begin)
                h_yz(
                    part,
                    x,
                    begin,
                    ef[2 + part, x + 1, where, :],
                    ef[4 + part, x + 1, where, :],
                )
        fill_h_edge(x)
        return carry

    def e_row(drive, x, carry):
        for tile in range(tiles):
            begin = tile * TILE
            where = pl.ds(begin + TILE, TILE)
            for part in range(2):
                e_x(part, x, begin, drive)
                e_yz(
                    part,
                    x,
                    begin,
                    hf[2 + part, x - 1, where, :],
                    hf[4 + part, x - 1, where, :],
                )
        fill_e_edge(x)
        return carry

    def e_boundary(step, chunk, carry):
        h_copy(chunk).wait()
        for tile in range(CHUNK // TILE):
            begin = pl.multiple_of(chunk * CHUNK + tile * TILE, TILE)
            hy_x = turned_pair(h_from, 0, pl.ds(begin, TILE), start_cos, start_sin)
            hz_x = turned_pair(h_from, 2, pl.ds(begin, TILE), start_cos, start_sin)
            for part in range(2):
                e_yz(part, 0, begin, hy_x[part], hz_x[part])

        @pl.when(step < steps - 1)
        def _():
            e_copy(chunk).start()

        return carry

    h_store = pltpu.make_async_copy(hf.at[:, :, pl.ds(TILE, width)], h_out.at[0], store_sem.at[0])
    e_store = pltpu.make_async_copy(ef.at[:, :, pl.ds(0, width)], e_out.at[0], store_sem.at[1])

    def advance(step, carry):
        drive = waveform[step]
        lax.fori_loop(0, chunks, h_boundary, 0)
        for tile in range(tiles):
            for part in range(2):
                h_x(part, last, tile * TILE)
        fill_h_edge(last)
        lax.fori_loop(0, last, h_row, 0)

        @pl.when(step == steps - 1)
        def _():
            h_store.start()

        lax.fori_loop(0, chunks, functools.partial(e_boundary, step), 0)
        for tile in range(tiles):
            for part in range(2):
                e_x(part, 0, tile * TILE, drive)
        fill_e_edge(0)
        lax.fori_loop(1, rows, functools.partial(e_row, drive), 0)
        return carry

    for snap in range(NSNAP):
        lax.fori_loop(snap * INTERVAL, (snap + 1) * INTERVAL, advance, 0)
        if snap == NSNAP - 1:
            e_store.start()

        def add_power(x, total):
            for part in range(4):
                for tile in range(tiles):
                    values = ef[part, x, pl.ds(tile * TILE, TILE), :]
                    total = total + values * values
            return total

        total = lax.fori_loop(0, rows, add_power, jnp.zeros((TILE, depth), F32))
        power_out[snap] = jnp.where(lane == PML + 6, total, 0.0)

    e_store.wait()
    h_store.wait()


def on_device(
    bloch_index,
    material,
    permittivity,
    absorption_peak,
    source_sheet,
    waveform,
    electric_in,
    magnetic_in,
):
    rows, width, depth = material.shape
    slabs = lax.axis_size("sp")
    angles = 2.0 * jnp.pi * bloch_index.astype(F32) / MPHASE
    trig = jnp.stack([jnp.cos(angles[0]), jnp.sin(angles[0])], 1).reshape(4)
    smem = pl.BlockSpec(memory_space=pltpu.SMEM)
    vmem = pl.BlockSpec(memory_space=pltpu.VMEM)
    hbm = pl.BlockSpec(memory_space=pl.ANY)
    chunks = width // CHUNK
    pair = pltpu.SemaphoreType.DMA((chunks,))
    electric_out, magnetic_out, power = pl.pallas_call(
        functools.partial(kernel, slabs, rows, width, depth),
        out_shape=(
            jax.ShapeDtypeStruct(electric_in.shape, F32),
            jax.ShapeDtypeStruct(magnetic_in.shape, F32),
            jax.ShapeDtypeStruct((NSNAP, TILE, depth), F32),
        ),
        in_specs=[smem, smem, smem, smem, vmem, hbm, hbm, hbm],
        out_specs=(hbm, hbm, vmem),
        scratch_shapes=[
            pltpu.VMEM((6, rows, width + TILE, depth), F32),
            pltpu.VMEM((6, rows, width + TILE, depth), F32),
            pltpu.VMEM((6, rows, width, depth), jnp.bfloat16),
            pltpu.VMEM((6, rows, width, depth), jnp.bfloat16),
            pltpu.VMEM((rows, width, depth), jnp.int32),
            pltpu.VMEM((rows, width, depth), F32),
            pltpu.VMEM((rows, width, depth), F32),
            pltpu.VMEM((2, rows, width, depth), F32),
            pltpu.VMEM((4, width, depth), F32),
            pltpu.VMEM((4, width, depth), F32),
            pltpu.SemaphoreType.DMA((5,)),
            pltpu.SemaphoreType.DMA((2,)),
            pair,
            pair,
            pair,
            pair,
        ],
        compiler_params=pltpu.CompilerParams(
            collective_id=0, has_side_effects=True, vmem_limit_bytes=40 * 2**20
        ),
        name="yee",
    )(
        trig,
        permittivity,
        absorption_peak,
        waveform,
        source_sheet,
        material,
        electric_in,
        magnetic_in,
    )
    cells_plane = rows * slabs * width
    reports = (jnp.sum(power, (1, 2)) / cells_plane)[None]
    reflected = of_everyone(reports, "sp")
    total_points = lax.axis_size("ka")
    reflected_mean = of_everyone(jnp.sum(reflected, 0) / total_points, "ka")
    return (electric_out, magnetic_out, reflected, reflected_mean)


def solution(mesh):
    in_specs = (
        P("ka", None),
        P("sp", None, None),
        P(),
        P(),
        P("ka", None, "sp", None),
        P(),
        P("ka", None, "sp", None, None),
        P("ka", None, "sp", None, None),
    )
    out_specs = (
        P("ka", None, "sp", None, None),
        P("ka", None, "sp", None, None),
        P("ka", None),
        P(),
    )
    return jax.shard_map(
        on_device, mesh=mesh, in_specs=in_specs, out_specs=out_specs, check_vma=False
    )
```

```python
import functools

import jax
import jax.numpy as jnp
from jax import lax
from jax.experimental import pallas as pl
from jax.experimental.pallas import tpu as pltpu
from jax.sharding import PartitionSpec as P

PML = 16
INTERVAL = 5
NSNAP = 2
MPHASE = 64
NMAT = 3
TIME_STEP = 0.5

MESH = pl.DeviceIdType.MESH
F32 = jnp.float32
TILE = 8


def kernel(
    sizes,
    bloch,
    permittivity,
    absorption_peak,
    waveform,
    sheet_in,
    material,
    e_in,
    h_in,
    e_out,
    h_out,
    reflected_out,
    mean_out,
    ef,
    hf,
    e_low,
    h_low,
    mat,
    keep,
    gain,
    sheet_raw,
    sheet,
    from_up,
    from_down,
    ghost_h,
    ghost_ex,
    ghost_kind,
    ghost_raw,
    ghost_keep,
    ghost_gain,
    ghost_sheet,
    my_kind,
    totals,
    slab_sums,
    point_sums,
    load_sem,
    up_send,
    up_recv,
    down_send,
    down_recv,
    ghost_send,
    ghost_recv,
    extra_send,
    extra_recv,
    slab_send,
    slab_recv,
    point_send,
    point_recv,
):
    points, slabs, rows, width, depth = sizes
    ka = lax.axis_index("ka")
    sp = lax.axis_index("sp")
    up = lax.rem(sp + 1, slabs)
    down = lax.rem(sp + slabs - 1, slabs)
    tiles = width // TILE
    last = rows - 1
    steps = NSNAP * INTERVAL
    inside = pl.ds(TILE, width)
    whole = pl.ds(0, width)

    barrier = pltpu.get_barrier_semaphore()
    for other in (up, down):
        pl.semaphore_signal(barrier, inc=1, device_id=(ka, other), device_id_type=MESH)

    def greet(offset, carry):
        peer = lax.rem(ka + offset, points)
        pl.semaphore_signal(barrier, inc=1, device_id=(peer, sp), device_id_type=MESH)
        return carry

    def load(source, target, index):
        copy = pltpu.make_async_copy(source, target, load_sem.at[index])
        copy.start()
        return copy

    middle = pl.ds(1, rows - 2)
    load_first = load(e_in.at[0, :, 0], e_low.at[:, 0], 0)
    load_last = load(e_in.at[0, :, last], e_low.at[:, last], 1)
    load_h_last = load(h_in.at[0, :, last], h_low.at[:, last], 2)
    load_mat_last = load(material.at[last], mat.at[last], 3)
    load_sheet = load(sheet_in.at[0], sheet_raw, 4)
    load_e = load(e_in.at[0, :, middle], e_low.at[:, middle], 5)
    load_h = load(h_in.at[0, :, pl.ds(0, last)], h_low.at[:, pl.ds(0, last)], 6)
    load_mat = load(material.at[pl.ds(0, last)], mat.at[pl.ds(0, last)], 7)
    lax.fori_loop(1, points, greet, 0)

    def remote(source, target, send, recv, other):
        return pltpu.make_async_remote_copy(
            src_ref=source,
            dst_ref=target,
            send_sem=send,
            recv_sem=recv,
            device_id=(ka, other),
            device_id_type=MESH,
        )

    def copy_up(slot, chunk):
        where = pl.ds(chunk * TILE, TILE)
        return remote(
            ef.at[pl.ds(2, 4), last, where],
            from_down.at[slot, :, where],
            up_send.at[chunk],
            up_recv.at[slot, chunk],
            up,
        )

    def copy_down(slot, chunk):
        where = pl.ds(chunk * TILE, TILE)
        return remote(
            ef.at[pl.ds(2, 4), 0, where],
            from_up.at[slot, :, where],
            down_send.at[chunk],
            down_recv.at[slot, chunk],
            down,
        )

    def copy_ghost(chunk):
        where = pl.ds((chunk + 1) * TILE, TILE)
        return remote(
            hf.at[pl.ds(2, 4), last, where],
            ghost_h.at[:, where],
            ghost_send.at[chunk],
            ghost_recv.at[chunk],
            up,
        )

    extras = [
        remote(
            ef.at[pl.ds(0, 2), last, whole],
            ghost_ex.at[:, whole],
            extra_send.at[0],
            extra_recv.at[0],
            up,
        ),
        remote(my_kind, ghost_kind, extra_send.at[1], extra_recv.at[1], up),
        remote(
            sheet_raw.at[:, pl.ds(rows - TILE, TILE)],
            ghost_raw,
            extra_send.at[2],
            extra_recv.at[2],
            up,
        ),
    ]

    load_first.wait()
    load_last.wait()
    for part in range(6):
        ef[part, last, whole, :] = e_low[part, last].astype(F32)
    for part in range(6):
        ef[part, 0, whole, :] = e_low[part, 0].astype(F32)
    load_h_last.wait()
    for part in range(6):
        hf[part, last, inside, :] = h_low[part, last].astype(F32)
    load_mat_last.wait()
    my_kind[...] = mat[last].astype(F32)
    load_sheet.wait()
    pl.semaphore_wait(barrier, points + 1)
    extras[0].start()
    for chunk in range(tiles):
        copy_up(0, chunk).start()
        copy_down(0, chunk).start()
        copy_ghost(chunk).start()
    extras[1].start()
    extras[2].start()

    angle_x = jnp.full((1, depth), 2.0 * jnp.pi * bloch[0, 0].astype(F32) / MPHASE, F32)
    angle_y = jnp.full((1, depth), 2.0 * jnp.pi * bloch[0, 1].astype(F32) / MPHASE, F32)
    cos_x, sin_x = jnp.cos(angle_x), jnp.sin(angle_x)
    cos_y, sin_y = jnp.cos(angle_y), jnp.sin(angle_y)
    at_end = sp == slabs - 1
    at_start = sp == 0
    end_cos = jnp.where(at_end, cos_x, 1.0)
    end_sin = jnp.where(at_end, sin_x, 0.0)
    start_cos = jnp.where(at_start, cos_x, 1.0)
    start_sin = jnp.where(at_start, -sin_x, 0.0)

    lane = lax.broadcasted_iota(jnp.int32, (TILE, depth), 1)
    at_top = lane == depth - 1
    at_bottom = lane == 0

    def z_above(values):
        return jnp.where(at_top, 0.0, pltpu.roll(values, depth - 1, 1))

    def z_below(values):
        return jnp.where(at_bottom, 0.0, pltpu.roll(values, 1, 1))

    height = lane.astype(F32)
    low_depth = jnp.maximum(PML - height, 0.0) / PML
    high_depth = jnp.maximum(height - (depth - 1 - PML), 0.0) / PML
    conduct = absorption_peak[0] * (low_depth**3 + high_depth**3)
    half_mag = conduct * (0.5 * TIME_STEP)
    h_keep = (1.0 - half_mag) / (1.0 + half_mag)
    h_gain = -TIME_STEP / (1.0 + half_mag)

    def rotate(pair, cosine, sine):
        return (pair[0] * cosine - pair[1] * sine, pair[0] * sine + pair[1] * cosine)

    def upper_edge(refs):
        first, edge = pl.ds(0, 1), pl.ds(width, 1)
        real, imag = rotate((refs[0][first, :], refs[1][first, :]), cos_y, sin_y)
        refs[0][edge, :] = real
        refs[1][edge, :] = imag

    def lower_edge(refs):
        end, edge = pl.ds(width + TILE - 1, 1), pl.ds(TILE - 1, 1)
        real, imag = rotate((refs[0][end, :], refs[1][end, :]), cos_y, -sin_y)
        refs[0][edge, :] = real
        refs[1][edge, :] = imag

    def fill_e_edge(x):
        for part in (0, 4):
            upper_edge((ef.at[part, x], ef.at[part + 1, x]))

    def fill_h_edge(x, parts=(0, 4)):
        for part in parts:
            lower_edge((hf.at[part, x], hf.at[part + 1, x]))

    def fill_ghost_ex_edge():
        upper_edge((ghost_ex.at[0], ghost_ex.at[1]))

    def fill_ghost_h_edge():
        lower_edge((ghost_h.at[2], ghost_h.at[3]))

    keeps = []
    gains = []
    for level in range(NMAT):
        relative = jnp.full((TILE, depth), permittivity[level], F32)
        half_ele = conduct * (0.5 * TIME_STEP) / relative
        keeps.append((1.0 - half_ele) / (1.0 + half_ele))
        gains.append(TIME_STEP / relative / (1.0 + half_ele))

    def choose(kind, table, zero, one):
        return jnp.where(kind == zero, table[0], jnp.where(kind == one, table[1], table[2]))

    load_e.wait()
    load_h.wait()
    load_mat.wait()

    def widen_e(x, carry):
        for part in range(6):
            ef[part, x, whole, :] = e_low[part, x].astype(F32)
        fill_e_edge(x)
        return carry

    def widen_h(x, carry):
        for part in range(6):
            hf[part, x, inside, :] = h_low[part, x].astype(F32)
        return carry

    def fill_coefficients(x, carry):
        for tile in range(tiles):
            where = pl.ds(tile * TILE, TILE)
            kind = mat[x, where, :]
            keep[x, where, :] = choose(kind, keeps, 0, 1)
            gain[x, where, :] = choose(kind, gains, 0, 1)
        return carry

    fill_e_edge(0)
    fill_e_edge(last)
    lax.fori_loop(1, last, widen_e, 0)
    lax.fori_loop(0, last, widen_h, 0)
    lax.fori_loop(0, rows, fill_coefficients, 0)

    at_sheet = lax.broadcasted_iota(jnp.int32, (width, depth), 1) == PML + 2
    for part in range(2):
        turned = sheet_raw[part].T
        for x in range(rows):
            spread = jnp.broadcast_to(turned[:, x : x + 1], (width, depth))
            sheet[part, x] = jnp.where(at_sheet, spread, 0.0)

    def h_x(part, x, begin):
        ey = ef[2 + part, x, pl.ds(begin, TILE), :]
        ez = ef[4 + part, x, pl.ds(begin, TILE), :]
        ez_y = ef[4 + part, x, pl.ds(begin + 1, TILE), :]
        change = (ez_y - ez) - (z_above(ey) - ey)
        where = pl.ds(begin + TILE, TILE)
        hf[part, x, where, :] = h_keep * hf[part, x, where, :] + h_gain * change

    def h_yz(part, x, begin, ey_x, ez_x):
        ex = ef[part, x, pl.ds(begin, TILE), :]
        ex_y = ef[part, x, pl.ds(begin + 1, TILE), :]
        ey = ef[2 + part, x, pl.ds(begin, TILE), :]
        ez = ef[4 + part, x, pl.ds(begin, TILE), :]
        where = pl.ds(begin + TILE, TILE)
        change_y = (z_above(ex) - ex) - (ez_x - ez)
        change_z = (ey_x - ey) - (ex_y - ex)
        hf[2 + part, x, where, :] = h_keep * hf[2 + part, x, where, :] + h_gain * change_y
        hf[4 + part, x, where, :] = h_keep * hf[4 + part, x, where, :] + h_gain * change_z

    def ghost_h_yz(part, begin, ey, ez):
        ex = ghost_ex[part, pl.ds(begin, TILE), :]
        ex_y = ghost_ex[part, pl.ds(begin + 1, TILE), :]
        ey_x = ef[2 + part, 0, pl.ds(begin, TILE), :]
        ez_x = ef[4 + part, 0, pl.ds(begin, TILE), :]
        where = pl.ds(begin + TILE, TILE)
        change_y = (z_above(ex) - ex) - (ez_x - ez)
        change_z = (ey_x - ey) - (ex_y - ex)
        ghost_h[part, where, :] = h_keep * ghost_h[part, where, :] + h_gain * change_y
        ghost_h[2 + part, where, :] = h_keep * ghost_h[2 + part, where, :] + h_gain * change_z

    def e_x(part, x, begin, drive):
        where = pl.ds(begin, TILE)
        hy = hf[2 + part, x, pl.ds(begin + TILE, TILE), :]
        hz = hf[4 + part, x, pl.ds(begin + TILE, TILE), :]
        hz_y = hf[4 + part, x, pl.ds(begin + TILE - 1, TILE), :]
        change = (hz - hz_y) - (hy - z_below(hy)) - drive * sheet[part, x, where, :]
        ef[part, x, where, :] = (
            keep[x, where, :] * ef[part, x, where, :] + gain[x, where, :] * change
        )

    def ghost_e_x(part, begin, drive):
        where = pl.ds(begin, TILE)
        hy = ghost_h[part, pl.ds(begin + TILE, TILE), :]
        hz = ghost_h[2 + part, pl.ds(begin + TILE, TILE), :]
        hz_y = ghost_h[2 + part, pl.ds(begin + TILE - 1, TILE), :]
        change = (hz - hz_y) - (hy - z_below(hy)) - drive * ghost_sheet[part, where, :]
        ghost_ex[part, where, :] = (
            ghost_keep[where, :] * ghost_ex[part, where, :] + ghost_gain[where, :] * change
        )

    def e_yz(part, x, begin, hy_x, hz_x):
        where = pl.ds(begin, TILE)
        hx = hf[part, x, pl.ds(begin + TILE, TILE), :]
        hx_y = hf[part, x, pl.ds(begin + TILE - 1, TILE), :]
        hy = hf[2 + part, x, pl.ds(begin + TILE, TILE), :]
        hz = hf[4 + part, x, pl.ds(begin + TILE, TILE), :]
        change_y = (hx - z_below(hx)) - (hz - hz_x)
        change_z = (hy - hy_x) - (hx - hx_y)
        retain = keep[x, where, :]
        factor = gain[x, where, :]
        ef[2 + part, x, where, :] = retain * ef[2 + part, x, where, :] + factor * change_y
        ef[4 + part, x, where, :] = retain * ef[4 + part, x, where, :] + factor * change_z

    def h_row(x, carry):
        for tile in range(tiles):
            begin = tile * TILE
            where = pl.ds(begin, TILE)
            for part in range(2):
                h_x(part, x, begin)
                h_yz(
                    part, x, begin, ef[2 + part, x + 1, where, :], ef[4 + part, x + 1, where, :]
                )
        fill_h_edge(x)
        return carry

    def h_row_out(x, carry):
        h_row(x, carry)
        for part in range(6):
            h_out[0, part, x] = hf[part, x, inside, :]
        return carry

    def e_row(drive, x, carry):
        for tile in range(tiles):
            begin = tile * TILE
            where = pl.ds(begin + TILE, TILE)
            for part in range(2):
                e_x(part, x, begin, drive)
                e_yz(
                    part, x, begin, hf[2 + part, x - 1, where, :], hf[4 + part, x - 1, where, :]
                )
        fill_e_edge(x)
        return carry

    def add_power(index, x):
        total = totals[index]
        for part in range(4):
            for tile in range(tiles):
                values = ef[part, x, pl.ds(tile * TILE, TILE), :]
                total = total + values * values
        totals[index] = total

    def e_row_out(drive, x, carry):
        e_row(drive, x, carry)
        for part in range(6):
            e_out[0, part, x] = ef[part, x, whole, :]
        add_power(NSNAP - 1, x)
        return carry

    def e_x_ends(drive):
        for x in (0, last):
            for tile in range(tiles):
                for part in range(2):
                    e_x(part, x, tile * TILE, drive)

    def finish_electric(drive):
        fill_h_edge(last, (4,))
        fill_ghost_h_edge()
        for tile in range(tiles):
            for part in range(2):
                ghost_e_x(part, tile * TILE, drive)
        fill_ghost_ex_edge()
        e_x_ends(drive)
        fill_e_edge(0)
        fill_e_edge(last)
        e_row(drive, 1, 0)
        e_row(drive, last - 1, 0)

    def begin_magnetic():
        h_row(0, 0)
        h_row(last - 1, 0)
        for tile in range(tiles):
            for part in range(2):
                h_x(part, last, tile * TILE)
        fill_h_edge(last, (0,))

    def pair_of(ref, part, where):
        return (ref[part, where, :], ref[part + 1, where, :])

    def receive(slot, chunk):
        arriving_up = copy_up(slot, chunk)
        arriving_down = copy_down(slot, chunk)
        arriving_up.wait()
        arriving_down.wait()
        begin = chunk * TILE
        where = pl.ds(begin, TILE)
        ey_up = rotate(pair_of(from_up.at[slot], 0, where), end_cos, end_sin)
        ez_up = rotate(pair_of(from_up.at[slot], 2, where), end_cos, end_sin)
        ey_down = rotate(pair_of(from_down.at[slot], 0, where), start_cos, start_sin)
        ez_down = rotate(pair_of(from_down.at[slot], 2, where), start_cos, start_sin)
        beyond = pl.ds(begin + TILE, TILE)
        for part in range(2):
            h_yz(part, last, begin, ey_up[part], ez_up[part])
            ghost_h_yz(part, begin, ey_down[part], ez_down[part])
        for part in range(2):
            e_yz(part, last, begin, hf[2 + part, last - 1, beyond, :], hf[4 + part, last - 1, beyond, :])
            e_yz(part, 0, begin, ghost_h[part, beyond, :], ghost_h[2 + part, beyond, :])

    def share(first, end, part, pieces):
        count = end - first
        return first + count * part // pieces, first + count * (part + 1) // pieces

    totals[...] = jnp.zeros(totals.shape, F32)

    extras[0].wait()
    real, imag = rotate((ghost_ex[0, whole, :], ghost_ex[1, whole, :]), start_cos, start_sin)
    ghost_ex[0, whole, :] = real
    ghost_ex[1, whole, :] = imag
    fill_ghost_ex_edge()

    def finish_ghost():
        extras[1].wait()
        extras[2].wait()
        for tile in range(tiles):
            where = pl.ds(tile * TILE, TILE)
            kind = ghost_kind[where, :]
            ghost_keep[where, :] = choose(kind, keeps, 0.0, 1.0)
            ghost_gain[where, :] = choose(kind, gains, 0.0, 1.0)
        real, imag = rotate(
            (ghost_raw[0], ghost_raw[1]), start_cos[:, :width], start_sin[:, :width]
        )
        for part, raw in enumerate((real, imag)):
            column = raw.T[:, TILE - 1 : TILE]
            spread = jnp.broadcast_to(column, (width, depth))
            ghost_sheet[part] = jnp.where(at_sheet, spread, 0.0)

    half = tiles // 2

    def advance(step, carry):
        slot = lax.rem(step, 2)
        drive = waveform[jnp.maximum(step - 1, 0)]

        @pl.when(step > 0)
        def _():
            finish_electric(drive)

        @pl.when(step == INTERVAL)
        def _():
            for x in (0, 1, last - 1, last):
                add_power(0, x)

        begin_magnetic()
        for chunk in range(tiles):

            @pl.when(step == 0)
            def _():
                copy_ghost(chunk).wait()
                where = pl.ds((chunk + 1) * TILE, TILE)
                for part in (0, 2):
                    real, imag = rotate(pair_of(ghost_h, part, where), start_cos, start_sin)
                    ghost_h[part, where, :] = real
                    ghost_h[part + 1, where, :] = imag

            receive(slot, chunk)
            copy_up(1 - slot, chunk).start()
            copy_down(1 - slot, chunk).start()
            if chunk < half:

                @pl.when(step > 0)
                def _():
                    begin, end = share(2, last - 1, chunk, half)
                    lax.fori_loop(begin, end, functools.partial(e_row, drive), 0)

            else:
                begin, end = share(1, last - 1, chunk - half, tiles - half)
                lax.fori_loop(begin, end, h_row, 0)

        @pl.when(step == INTERVAL)
        def _():
            def add(x, inner):
                add_power(0, x)
                return inner

            lax.fori_loop(2, last - 1, add, 0)

        @pl.when(step == 0)
        def _():
            finish_ghost()

        return carry

    lax.fori_loop(0, steps - 1, advance, 0)

    slot = (steps - 1) % 2
    drive = waveform[steps - 2]
    finish_electric(drive)
    lax.fori_loop(2, last - 1, functools.partial(e_row, drive), 0)
    begin_magnetic()
    lax.fori_loop(1, last - 1, h_row_out, 0)
    for x in (0, last - 1):
        for part in range(6):
            h_out[0, part, x] = hf[part, x, inside, :]
    final = waveform[steps - 1]
    lax.fori_loop(1, last, functools.partial(e_row_out, final), 0)
    for chunk in range(tiles):
        receive(slot, chunk)
    fill_h_edge(last, (4,))
    e_x_ends(final)
    add_power(NSNAP - 1, 0)
    add_power(NSNAP - 1, last)

    row_index = lax.broadcasted_iota(jnp.int32, (TILE, depth), 0)
    at_monitor = lane == PML + 6
    mine = jnp.zeros((TILE, depth), F32)
    for snap in range(NSNAP):
        mine = jnp.where(row_index == snap, jnp.sum(jnp.where(at_monitor, totals[snap], 0.0)), mine)
    slab_sums[0] = mine

    def slab_copy(offset):
        return remote(
            slab_sums.at[0],
            slab_sums.at[offset],
            slab_send.at[offset],
            slab_recv.at[offset],
            lax.rem(sp + offset, slabs),
        )

    def point_copy(offset):
        return pltpu.make_async_remote_copy(
            src_ref=point_sums.at[0],
            dst_ref=point_sums.at[offset],
            send_sem=point_send.at[offset],
            recv_sem=point_recv.at[offset],
            device_id=(lax.rem(ka + offset, points), sp),
            device_id_type=MESH,
        )

    def started(copy):
        def start(offset, carry):
            copy(offset).start()
            return carry

        return start

    def waited(copy):
        def wait(offset, carry):
            copy(offset).wait()
            return carry

        return wait

    lax.fori_loop(1, slabs, started(slab_copy), 0)
    for x in (0, last):
        for part in range(6):
            e_out[0, part, x] = ef[part, x, whole, :]
    for part in range(6):
        h_out[0, part, last] = hf[part, last, inside, :]
    lax.fori_loop(1, slabs, waited(slab_copy), 0)
    total = slab_sums[0]
    for offset in range(1, slabs):
        total = total + slab_sums[offset]
    total = total / (rows * slabs * width)
    point_sums[0] = total
    reflected_out[...] = total
    lax.fori_loop(1, points, started(point_copy), 0)
    lax.fori_loop(1, points, waited(point_copy), 0)
    total = point_sums[0]
    for offset in range(1, points):
        total = total + point_sums[offset]
    mean_out[...] = total / points


def on_device(
    bloch_index,
    material,
    permittivity,
    absorption_peak,
    source_sheet,
    waveform,
    electric_in,
    magnetic_in,
):
    rows, width, depth = material.shape
    slabs = lax.axis_size("sp")
    points = lax.axis_size("ka")
    tiles = width // TILE
    smem = pl.BlockSpec(memory_space=pltpu.SMEM)
    vmem = pl.BlockSpec(memory_space=pltpu.VMEM)
    hbm = pl.BlockSpec(memory_space=pltpu.HBM)
    dma = pltpu.SemaphoreType.DMA
    tile = jax.ShapeDtypeStruct((TILE, depth), F32)
    electric_out, magnetic_out, reflected, mean = pl.pallas_call(
        functools.partial(kernel, (points, slabs, rows, width, depth)),
        out_shape=(
            jax.ShapeDtypeStruct(electric_in.shape, F32),
            jax.ShapeDtypeStruct(magnetic_in.shape, F32),
            tile,
            tile,
        ),
        in_specs=[smem, smem, smem, smem, hbm, hbm, hbm, hbm],
        out_specs=(vmem, vmem, vmem, vmem),
        scratch_shapes=[
            pltpu.VMEM((6, rows, width + TILE, depth), F32),
            pltpu.VMEM((6, rows, width + TILE, depth), F32),
            pltpu.VMEM((6, rows, width, depth), jnp.bfloat16),
            pltpu.VMEM((6, rows, width, depth), jnp.bfloat16),
            pltpu.VMEM((rows, width, depth), jnp.int32),
            pltpu.VMEM((rows, width, depth), F32),
            pltpu.VMEM((rows, width, depth), F32),
            pltpu.VMEM((2, rows, width), F32),
            pltpu.VMEM((2, rows, width, depth), F32),
            pltpu.VMEM((2, 4, width, depth), F32),
            pltpu.VMEM((2, 4, width, depth), F32),
            pltpu.VMEM((4, width + TILE, depth), F32),
            pltpu.VMEM((2, width + TILE, depth), F32),
            pltpu.VMEM((width, depth), F32),
            pltpu.VMEM((2, TILE, width), F32),
            pltpu.VMEM((width, depth), F32),
            pltpu.VMEM((width, depth), F32),
            pltpu.VMEM((2, width, depth), F32),
            pltpu.VMEM((width, depth), F32),
            pltpu.VMEM((NSNAP, TILE, depth), F32),
            pltpu.VMEM((slabs, TILE, depth), F32),
            pltpu.VMEM((points, TILE, depth), F32),
            dma((8,)),
            dma((tiles,)),
            dma((2, tiles)),
            dma((tiles,)),
            dma((2, tiles)),
            dma((tiles,)),
            dma((tiles,)),
            dma((3,)),
            dma((3,)),
            dma((slabs,)),
            dma((slabs,)),
            dma((points,)),
            dma((points,)),
        ],
        compiler_params=pltpu.CompilerParams(
            collective_id=0, has_side_effects=True, vmem_limit_bytes=32 * 2**20
        ),
        name="yee",
    )(
        bloch_index,
        permittivity,
        absorption_peak,
        waveform,
        source_sheet,
        material,
        electric_in,
        magnetic_in,
    )
    return (electric_out, magnetic_out, reflected[None, :NSNAP, 0], mean[:NSNAP, 0])


def solution(mesh):
    in_specs = (
        P("ka", None),
        P("sp", None, None),
        P(),
        P(),
        P("ka", None, "sp", None),
        P(),
        P("ka", None, "sp", None, None),
        P("ka", None, "sp", None, None),
    )
    out_specs = (
        P("ka", None, "sp", None, None),
        P("ka", None, "sp", None, None),
        P("ka", None),
        P(),
    )
    return jax.shard_map(
        on_device, mesh=mesh, in_specs=in_specs, out_specs=out_specs, check_vma=False
    )
```

```python
import functools

import jax
import jax.numpy as jnp
from jax import lax
from jax.experimental import pallas as pl
from jax.experimental.pallas import tpu as pltpu
from jax.sharding import PartitionSpec as P

PML = 16
INTERVAL = 5
NSNAP = 2
MPHASE = 64
NMAT = 3
TIME_STEP = 0.5

MESH = pl.DeviceIdType.MESH
F32 = jnp.float32
TILE = 8


def kernel(
    sizes,
    bloch_in,
    permittivity_in,
    absorption_peak,
    waveform_in,
    sheet_in,
    material,
    e_in,
    h_in,
    e_out,
    h_out,
    reflected_out,
    mean_out,
    bloch,
    permittivity,
    waveform,
    ef,
    hf,
    e_low,
    h_low,
    mat,
    keep,
    gain,
    sheet_raw,
    sheet,
    from_up,
    from_down,
    ghost_h,
    ghost_ex,
    ghost_kind,
    ghost_raw,
    ghost_keep,
    ghost_gain,
    ghost_sheet,
    my_kind,
    totals,
    slab_sums,
    point_sums,
    load_sem,
    up_send,
    up_recv,
    down_send,
    down_recv,
    ghost_send,
    ghost_recv,
    extra_send,
    extra_recv,
    slab_send,
    slab_recv,
    point_send,
    point_recv,
    hello,
):
    points, slabs, rows, width, depth = sizes
    ka = lax.axis_index("ka")
    sp = lax.axis_index("sp")
    up = lax.rem(sp + 1, slabs)
    down = lax.rem(sp + slabs - 1, slabs)
    tiles = width // TILE
    last = rows - 1
    steps = NSNAP * INTERVAL
    inside = pl.ds(TILE, width)
    whole = pl.ds(0, width)

    z_above_1 = lax.rem(ka + 4, points)
    z_below_1 = lax.rem(ka + points - 4, points)
    z_above_2 = lax.rem(ka + 8, points)
    z_below_2 = lax.rem(ka + points - 8, points)
    core_peer = ka + 1 - 2 * lax.rem(ka, 2)
    x_peer = ka + 2 - 4 * lax.rem(ka // 2, 2)

    barrier = pltpu.get_barrier_semaphore()
    near = [(ka, up), (ka, down)]
    near += [(peer, sp) for peer in (z_above_1, z_below_1, core_peer, x_peer)]
    for device in near:
        pl.semaphore_signal(barrier, inc=1, device_id=device, device_id_type=MESH)

    rounds = [
        ((0, z_above_1), (1, z_below_1)),
        ((2, z_above_2), (3, z_below_2)),
        ((4, core_peer),),
        ((5, x_peer),),
    ]

    def greet(step):
        for index in range(len(rounds) + 1):

            @pl.when(step == index)
            def _():
                if index > 0:
                    for place, _peer in rounds[index - 1]:
                        pl.semaphore_wait(hello.at[place], 1)
                if index < len(rounds):
                    for place, peer in rounds[index]:
                        pl.semaphore_signal(
                            hello.at[place], inc=1, device_id=(peer, sp), device_id_type=MESH
                        )

    def load(source, target, index):
        copy = pltpu.make_async_copy(source, target, load_sem.at[index])
        copy.start()
        return copy

    middle = pl.ds(1, rows - 2)
    load_first = load(e_in.at[0, :, 0], e_low.at[:, 0], 0)
    load_last = load(e_in.at[0, :, last], e_low.at[:, last], 1)
    load_h_last = load(h_in.at[0, :, last], h_low.at[:, last], 2)
    load_mat_last = load(material.at[last], mat.at[last], 3)
    load_sheet = load(sheet_in.at[0], sheet_raw, 4)
    load_e = load(e_in.at[0, :, middle], e_low.at[:, middle], 5)
    load_h = load(h_in.at[0, :, pl.ds(0, last)], h_low.at[:, pl.ds(0, last)], 6)
    load_mat = load(material.at[pl.ds(0, last)], mat.at[pl.ds(0, last)], 7)
    small = [
        load(bloch_in, bloch, 8),
        load(permittivity_in, permittivity, 9),
        load(waveform_in, waveform, 10),
    ]

    def remote(source, target, send, recv, other):
        return pltpu.make_async_remote_copy(
            src_ref=source,
            dst_ref=target,
            send_sem=send,
            recv_sem=recv,
            device_id=(ka, other),
            device_id_type=MESH,
        )

    def copy_up(slot, chunk):
        where = pl.ds(chunk * TILE, TILE)
        return remote(
            ef.at[pl.ds(2, 4), last, where],
            from_down.at[slot, :, where],
            up_send.at[chunk],
            up_recv.at[slot, chunk],
            up,
        )

    def copy_down(slot, chunk):
        where = pl.ds(chunk * TILE, TILE)
        return remote(
            ef.at[pl.ds(2, 4), 0, where],
            from_up.at[slot, :, where],
            down_send.at[chunk],
            down_recv.at[slot, chunk],
            down,
        )

    def copy_ghost(chunk):
        where = pl.ds((chunk + 1) * TILE, TILE)
        return remote(
            hf.at[pl.ds(2, 4), last, where],
            ghost_h.at[:, where],
            ghost_send.at[chunk],
            ghost_recv.at[chunk],
            up,
        )

    extras = [
        remote(
            ef.at[pl.ds(0, 2), last, whole],
            ghost_ex.at[:, whole],
            extra_send.at[0],
            extra_recv.at[0],
            up,
        ),
        remote(my_kind, ghost_kind, extra_send.at[1], extra_recv.at[1], up),
        remote(
            sheet_raw.at[:, pl.ds(rows - TILE, TILE)],
            ghost_raw,
            extra_send.at[2],
            extra_recv.at[2],
            up,
        ),
    ]

    load_first.wait()
    load_last.wait()
    for part in range(6):
        ef[part, last, whole, :] = e_low[part, last].astype(F32)
    for part in range(6):
        ef[part, 0, whole, :] = e_low[part, 0].astype(F32)
    load_h_last.wait()
    for part in range(6):
        hf[part, last, inside, :] = h_low[part, last].astype(F32)
    load_mat_last.wait()
    my_kind[...] = mat[last].astype(F32)
    load_sheet.wait()
    pl.semaphore_wait(barrier, len(near))
    extras[0].start()
    for chunk in range(tiles):
        copy_up(0, chunk).start()
        copy_down(0, chunk).start()
        copy_ghost(chunk).start()
    extras[1].start()
    extras[2].start()
    for copy in small:
        copy.wait()

    angle_x = jnp.full((1, depth), 2.0 * jnp.pi * bloch[0, 0].astype(F32) / MPHASE, F32)
    angle_y = jnp.full((1, depth), 2.0 * jnp.pi * bloch[0, 1].astype(F32) / MPHASE, F32)
    cos_x, sin_x = jnp.cos(angle_x), jnp.sin(angle_x)
    cos_y, sin_y = jnp.cos(angle_y), jnp.sin(angle_y)
    at_end = sp == slabs - 1
    at_start = sp == 0
    end_cos = jnp.where(at_end, cos_x, 1.0)
    end_sin = jnp.where(at_end, sin_x, 0.0)
    start_cos = jnp.where(at_start, cos_x, 1.0)
    start_sin = jnp.where(at_start, -sin_x, 0.0)

    lane = lax.broadcasted_iota(jnp.int32, (TILE, depth), 1)
    at_top = lane == depth - 1
    at_bottom = lane == 0

    def z_above(values):
        return jnp.where(at_top, 0.0, pltpu.roll(values, depth - 1, 1))

    def z_below(values):
        return jnp.where(at_bottom, 0.0, pltpu.roll(values, 1, 1))

    height = lane.astype(F32)
    low_depth = jnp.maximum(PML - height, 0.0) / PML
    high_depth = jnp.maximum(height - (depth - 1 - PML), 0.0) / PML
    conduct = absorption_peak[0] * (low_depth**3 + high_depth**3)
    half_mag = conduct * (0.5 * TIME_STEP)
    h_keep = (1.0 - half_mag) / (1.0 + half_mag)
    h_gain = -TIME_STEP / (1.0 + half_mag)

    def rotate(pair, cosine, sine):
        return (pair[0] * cosine - pair[1] * sine, pair[0] * sine + pair[1] * cosine)

    def upper_edge(refs):
        first, edge = pl.ds(0, 1), pl.ds(width, 1)
        real, imag = rotate((refs[0][first, :], refs[1][first, :]), cos_y, sin_y)
        refs[0][edge, :] = real
        refs[1][edge, :] = imag

    def lower_edge(refs):
        end, edge = pl.ds(width + TILE - 1, 1), pl.ds(TILE - 1, 1)
        real, imag = rotate((refs[0][end, :], refs[1][end, :]), cos_y, -sin_y)
        refs[0][edge, :] = real
        refs[1][edge, :] = imag

    def fill_e_edge(x):
        for part in (0, 4):
            upper_edge((ef.at[part, x], ef.at[part + 1, x]))

    def fill_h_edge(x, parts=(0, 4)):
        for part in parts:
            lower_edge((hf.at[part, x], hf.at[part + 1, x]))

    def fill_ghost_ex_edge():
        upper_edge((ghost_ex.at[0], ghost_ex.at[1]))

    def fill_ghost_h_edge():
        lower_edge((ghost_h.at[2], ghost_h.at[3]))

    keeps = []
    gains = []
    for level in range(NMAT):
        relative = jnp.full((TILE, depth), permittivity[level], F32)
        half_ele = conduct * (0.5 * TIME_STEP) / relative
        keeps.append((1.0 - half_ele) / (1.0 + half_ele))
        gains.append(TIME_STEP / relative / (1.0 + half_ele))

    def choose(kind, table, zero, one):
        return jnp.where(kind == zero, table[0], jnp.where(kind == one, table[1], table[2]))

    load_e.wait()
    load_h.wait()
    load_mat.wait()

    def widen_e(x, carry):
        for part in range(6):
            ef[part, x, whole, :] = e_low[part, x].astype(F32)
        fill_e_edge(x)
        return carry

    def widen_h(x, carry):
        for part in range(6):
            hf[part, x, inside, :] = h_low[part, x].astype(F32)
        return carry

    def fill_coefficients(x, carry):
        for tile in range(tiles):
            where = pl.ds(tile * TILE, TILE)
            kind = mat[x, where, :]
            keep[x, where, :] = choose(kind, keeps, 0, 1)
            gain[x, where, :] = choose(kind, gains, 0, 1)
        return carry

    fill_e_edge(0)
    fill_e_edge(last)
    lax.fori_loop(1, last, widen_e, 0)
    lax.fori_loop(0, last, widen_h, 0)
    lax.fori_loop(0, rows, fill_coefficients, 0)

    at_sheet = lax.broadcasted_iota(jnp.int32, (width, depth), 1) == PML + 2
    for part in range(2):
        turned = sheet_raw[part].T
        for x in range(rows):
            spread = jnp.broadcast_to(turned[:, x : x + 1], (width, depth))
            sheet[part, x] = jnp.where(at_sheet, spread, 0.0)

    def h_x(part, x, begin):
        ey = ef[2 + part, x, pl.ds(begin, TILE), :]
        ez = ef[4 + part, x, pl.ds(begin, TILE), :]
        ez_y = ef[4 + part, x, pl.ds(begin + 1, TILE), :]
        change = (ez_y - ez) - (z_above(ey) - ey)
        where = pl.ds(begin + TILE, TILE)
        hf[part, x, where, :] = h_keep * hf[part, x, where, :] + h_gain * change

    def h_yz(part, x, begin, ey_x, ez_x):
        ex = ef[part, x, pl.ds(begin, TILE), :]
        ex_y = ef[part, x, pl.ds(begin + 1, TILE), :]
        ey = ef[2 + part, x, pl.ds(begin, TILE), :]
        ez = ef[4 + part, x, pl.ds(begin, TILE), :]
        where = pl.ds(begin + TILE, TILE)
        change_y = (z_above(ex) - ex) - (ez_x - ez)
        change_z = (ey_x - ey) - (ex_y - ex)
        hf[2 + part, x, where, :] = h_keep * hf[2 + part, x, where, :] + h_gain * change_y
        hf[4 + part, x, where, :] = h_keep * hf[4 + part, x, where, :] + h_gain * change_z

    def ghost_h_yz(part, begin, ey, ez):
        ex = ghost_ex[part, pl.ds(begin, TILE), :]
        ex_y = ghost_ex[part, pl.ds(begin + 1, TILE), :]
        ey_x = ef[2 + part, 0, pl.ds(begin, TILE), :]
        ez_x = ef[4 + part, 0, pl.ds(begin, TILE), :]
        where = pl.ds(begin + TILE, TILE)
        change_y = (z_above(ex) - ex) - (ez_x - ez)
        change_z = (ey_x - ey) - (ex_y - ex)
        ghost_h[part, where, :] = h_keep * ghost_h[part, where, :] + h_gain * change_y
        ghost_h[2 + part, where, :] = h_keep * ghost_h[2 + part, where, :] + h_gain * change_z

    def e_x(part, x, begin, drive):
        where = pl.ds(begin, TILE)
        hy = hf[2 + part, x, pl.ds(begin + TILE, TILE), :]
        hz = hf[4 + part, x, pl.ds(begin + TILE, TILE), :]
        hz_y = hf[4 + part, x, pl.ds(begin + TILE - 1, TILE), :]
        change = (hz - hz_y) - (hy - z_below(hy)) - drive * sheet[part, x, where, :]
        ef[part, x, where, :] = (
            keep[x, where, :] * ef[part, x, where, :] + gain[x, where, :] * change
        )

    def ghost_e_x(part, begin, drive):
        where = pl.ds(begin, TILE)
        hy = ghost_h[part, pl.ds(begin + TILE, TILE), :]
        hz = ghost_h[2 + part, pl.ds(begin + TILE, TILE), :]
        hz_y = ghost_h[2 + part, pl.ds(begin + TILE - 1, TILE), :]
        change = (hz - hz_y) - (hy - z_below(hy)) - drive * ghost_sheet[part, where, :]
        ghost_ex[part, where, :] = (
            ghost_keep[where, :] * ghost_ex[part, where, :] + ghost_gain[where, :] * change
        )

    def e_yz(part, x, begin, hy_x, hz_x):
        where = pl.ds(begin, TILE)
        hx = hf[part, x, pl.ds(begin + TILE, TILE), :]
        hx_y = hf[part, x, pl.ds(begin + TILE - 1, TILE), :]
        hy = hf[2 + part, x, pl.ds(begin + TILE, TILE), :]
        hz = hf[4 + part, x, pl.ds(begin + TILE, TILE), :]
        change_y = (hx - z_below(hx)) - (hz - hz_x)
        change_z = (hy - hy_x) - (hx - hx_y)
        retain = keep[x, where, :]
        factor = gain[x, where, :]
        ef[2 + part, x, where, :] = retain * ef[2 + part, x, where, :] + factor * change_y
        ef[4 + part, x, where, :] = retain * ef[4 + part, x, where, :] + factor * change_z

    def h_row(x, carry):
        for tile in range(tiles):
            begin = tile * TILE
            where = pl.ds(begin, TILE)
            for part in range(2):
                h_x(part, x, begin)
                h_yz(
                    part, x, begin, ef[2 + part, x + 1, where, :], ef[4 + part, x + 1, where, :]
                )
        fill_h_edge(x)
        return carry

    def h_row_out(x, carry):
        h_row(x, carry)
        for part in range(6):
            h_out[0, part, x] = hf[part, x, inside, :]
        return carry

    def e_row(drive, x, carry):
        for tile in range(tiles):
            begin = tile * TILE
            where = pl.ds(begin + TILE, TILE)
            for part in range(2):
                e_x(part, x, begin, drive)
                e_yz(
                    part, x, begin, hf[2 + part, x - 1, where, :], hf[4 + part, x - 1, where, :]
                )
        fill_e_edge(x)
        return carry

    def add_power(index, x):
        total = totals[index]
        for part in range(4):
            for tile in range(tiles):
                values = ef[part, x, pl.ds(tile * TILE, TILE), :]
                total = total + values * values
        totals[index] = total

    def e_row_out(drive, x, carry):
        e_row(drive, x, carry)
        for part in range(6):
            e_out[0, part, x] = ef[part, x, whole, :]
        add_power(NSNAP - 1, x)
        return carry

    def e_x_ends(drive):
        for x in (0, last):
            for tile in range(tiles):
                for part in range(2):
                    e_x(part, x, tile * TILE, drive)

    def finish_electric(drive):
        fill_h_edge(last, (4,))
        fill_ghost_h_edge()
        for tile in range(tiles):
            for part in range(2):
                ghost_e_x(part, tile * TILE, drive)
        fill_ghost_ex_edge()
        e_x_ends(drive)
        fill_e_edge(0)
        fill_e_edge(last)
        e_row(drive, 1, 0)
        e_row(drive, last - 1, 0)

    def begin_magnetic():
        h_row(0, 0)
        h_row(last - 1, 0)
        for tile in range(tiles):
            for part in range(2):
                h_x(part, last, tile * TILE)
        fill_h_edge(last, (0,))

    def pair_of(ref, part, where):
        return (ref[part, where, :], ref[part + 1, where, :])

    def receive(slot, chunk):
        arriving_up = copy_up(slot, chunk)
        arriving_down = copy_down(slot, chunk)
        arriving_up.wait()
        arriving_down.wait()
        begin = chunk * TILE
        where = pl.ds(begin, TILE)
        ey_up = rotate(pair_of(from_up.at[slot], 0, where), end_cos, end_sin)
        ez_up = rotate(pair_of(from_up.at[slot], 2, where), end_cos, end_sin)
        ey_down = rotate(pair_of(from_down.at[slot], 0, where), start_cos, start_sin)
        ez_down = rotate(pair_of(from_down.at[slot], 2, where), start_cos, start_sin)
        beyond = pl.ds(begin + TILE, TILE)
        for part in range(2):
            h_yz(part, last, begin, ey_up[part], ez_up[part])
            ghost_h_yz(part, begin, ey_down[part], ez_down[part])
        for part in range(2):
            e_yz(part, last, begin, hf[2 + part, last - 1, beyond, :], hf[4 + part, last - 1, beyond, :])
            e_yz(part, 0, begin, ghost_h[part, beyond, :], ghost_h[2 + part, beyond, :])

    def share(first, end, part, pieces):
        count = end - first
        return first + count * part // pieces, first + count * (part + 1) // pieces

    totals[...] = jnp.zeros(totals.shape, F32)

    extras[0].wait()
    real, imag = rotate((ghost_ex[0, whole, :], ghost_ex[1, whole, :]), start_cos, start_sin)
    ghost_ex[0, whole, :] = real
    ghost_ex[1, whole, :] = imag
    fill_ghost_ex_edge()

    def finish_ghost():
        extras[1].wait()
        extras[2].wait()
        for tile in range(tiles):
            where = pl.ds(tile * TILE, TILE)
            kind = ghost_kind[where, :]
            ghost_keep[where, :] = choose(kind, keeps, 0.0, 1.0)
            ghost_gain[where, :] = choose(kind, gains, 0.0, 1.0)
        real, imag = rotate(
            (ghost_raw[0], ghost_raw[1]), start_cos[:, :width], start_sin[:, :width]
        )
        for part, raw in enumerate((real, imag)):
            column = raw.T[:, TILE - 1 : TILE]
            spread = jnp.broadcast_to(column, (width, depth))
            ghost_sheet[part] = jnp.where(at_sheet, spread, 0.0)

    half = tiles // 2

    def advance(step, carry):
        slot = lax.rem(step, 2)
        drive = waveform[jnp.maximum(step - 1, 0)]

        @pl.when(step > 0)
        def _():
            finish_electric(drive)

        @pl.when(step == INTERVAL)
        def _():
            for x in (0, 1, last - 1, last):
                add_power(0, x)

        begin_magnetic()
        greet(step)
        for chunk in range(tiles):

            @pl.when(step == 0)
            def _():
                copy_ghost(chunk).wait()
                where = pl.ds((chunk + 1) * TILE, TILE)
                for part in (0, 2):
                    real, imag = rotate(pair_of(ghost_h, part, where), start_cos, start_sin)
                    ghost_h[part, where, :] = real
                    ghost_h[part + 1, where, :] = imag

            receive(slot, chunk)
            copy_up(1 - slot, chunk).start()
            copy_down(1 - slot, chunk).start()
            if chunk < half:

                @pl.when(step > 0)
                def _():
                    begin, end = share(2, last - 1, chunk, half)
                    lax.fori_loop(begin, end, functools.partial(e_row, drive), 0)

            else:
                begin, end = share(1, last - 1, chunk - half, tiles - half)
                lax.fori_loop(begin, end, h_row, 0)

        @pl.when(step == INTERVAL)
        def _():
            def add(x, inner):
                add_power(0, x)
                return inner

            lax.fori_loop(2, last - 1, add, 0)

        @pl.when(step == 0)
        def _():
            finish_ghost()

        return carry

    lax.fori_loop(0, steps - 1, advance, 0)

    slot = (steps - 1) % 2
    drive = waveform[steps - 2]
    finish_electric(drive)
    lax.fori_loop(2, last - 1, functools.partial(e_row, drive), 0)
    begin_magnetic()
    lax.fori_loop(1, last - 1, h_row_out, 0)
    for x in (0, last - 1):
        for part in range(6):
            h_out[0, part, x] = hf[part, x, inside, :]
    final = waveform[steps - 1]
    lax.fori_loop(1, last, functools.partial(e_row_out, final), 0)
    for chunk in range(tiles):
        receive(slot, chunk)
    fill_h_edge(last, (4,))
    e_x_ends(final)
    add_power(NSNAP - 1, 0)
    add_power(NSNAP - 1, last)

    at_monitor = lane == PML + 6
    lane_row = lax.broadcasted_iota(jnp.int32, (1, depth), 1)
    mine = jnp.zeros((1, depth), F32)
    for snap in range(NSNAP):
        power = jnp.sum(jnp.where(at_monitor, totals[snap], 0.0))
        mine = jnp.where(lane_row == snap, power, mine)
    slab_sums[0] = mine

    def slab_copy(offset):
        return remote(
            slab_sums.at[0],
            slab_sums.at[offset],
            slab_send.at[offset],
            slab_recv.at[offset],
            lax.rem(sp + offset, slabs),
        )

    def point_copy(offset):
        return pltpu.make_async_remote_copy(
            src_ref=point_sums.at[0],
            dst_ref=point_sums.at[offset],
            send_sem=point_send.at[offset],
            recv_sem=point_recv.at[offset],
            device_id=(lax.rem(ka + offset, points), sp),
            device_id_type=MESH,
        )

    def started(copy):
        def start(offset, carry):
            copy(offset).start()
            return carry

        return start

    def waited(copy):
        def wait(offset, carry):
            copy(offset).wait()
            return carry

        return wait

    lax.fori_loop(1, slabs, started(slab_copy), 0)
    for x in (0, last):
        for part in range(6):
            e_out[0, part, x] = ef[part, x, whole, :]
    for part in range(6):
        h_out[0, part, last] = hf[part, last, inside, :]
    lax.fori_loop(1, slabs, waited(slab_copy), 0)
    total = slab_sums[0]
    for offset in range(1, slabs):
        total = total + slab_sums[offset]
    total = total / (rows * slabs * width)
    point_sums[0] = total
    reflected_out[...] = total
    lax.fori_loop(1, points, started(point_copy), 0)
    lax.fori_loop(1, points, waited(point_copy), 0)
    total = point_sums[0]
    for offset in range(1, points):
        total = total + point_sums[offset]
    mean_out[...] = total / points


def in_hbm(values):
    return pltpu.with_memory_space_constraint(values, pltpu.HBM)


def on_device(
    bloch_index,
    material,
    permittivity,
    absorption_peak,
    source_sheet,
    waveform,
    electric_in,
    magnetic_in,
):
    rows, width, depth = material.shape
    slabs = lax.axis_size("sp")
    points = lax.axis_size("ka")
    tiles = width // TILE
    vmem = pl.BlockSpec(memory_space=pltpu.VMEM)
    hbm = pl.BlockSpec(memory_space=pltpu.HBM)
    dma = pltpu.SemaphoreType.DMA
    row = jax.ShapeDtypeStruct((1, depth), F32)
    electric_out, magnetic_out, reflected, mean = pl.pallas_call(
        functools.partial(kernel, (points, slabs, rows, width, depth)),
        out_shape=(
            jax.ShapeDtypeStruct(electric_in.shape, F32),
            jax.ShapeDtypeStruct(magnetic_in.shape, F32),
            row,
            row,
        ),
        in_specs=[hbm, hbm, pl.BlockSpec(memory_space=pltpu.SMEM)] + [hbm] * 5,
        out_specs=(vmem, vmem, vmem, vmem),
        scratch_shapes=[
            pltpu.SMEM(bloch_index.shape, jnp.int32),
            pltpu.SMEM(permittivity.shape, F32),
            pltpu.SMEM(waveform.shape, F32),
            pltpu.VMEM((6, rows, width + TILE, depth), F32),
            pltpu.VMEM((6, rows, width + TILE, depth), F32),
            pltpu.VMEM((6, rows, width, depth), jnp.bfloat16),
            pltpu.VMEM((6, rows, width, depth), jnp.bfloat16),
            pltpu.VMEM((rows, width, depth), jnp.int32),
            pltpu.VMEM((rows, width, depth), F32),
            pltpu.VMEM((rows, width, depth), F32),
            pltpu.VMEM((2, rows, width), F32),
            pltpu.VMEM((2, rows, width, depth), F32),
            pltpu.VMEM((2, 4, width, depth), F32),
            pltpu.VMEM((2, 4, width, depth), F32),
            pltpu.VMEM((4, width + TILE, depth), F32),
            pltpu.VMEM((2, width + TILE, depth), F32),
            pltpu.VMEM((width, depth), F32),
            pltpu.VMEM((2, TILE, width), F32),
            pltpu.VMEM((width, depth), F32),
            pltpu.VMEM((width, depth), F32),
            pltpu.VMEM((2, width, depth), F32),
            pltpu.VMEM((width, depth), F32),
            pltpu.VMEM((NSNAP, TILE, depth), F32),
            pltpu.VMEM((slabs, 1, depth), F32),
            pltpu.VMEM((points, 1, depth), F32),
            dma((11,)),
            dma((tiles,)),
            dma((2, tiles)),
            dma((tiles,)),
            dma((2, tiles)),
            dma((tiles,)),
            dma((tiles,)),
            dma((3,)),
            dma((3,)),
            dma((slabs,)),
            dma((slabs,)),
            dma((points,)),
            dma((points,)),
            pltpu.SemaphoreType.REGULAR((6,)),
        ],
        compiler_params=pltpu.CompilerParams(
            collective_id=0, has_side_effects=True, vmem_limit_bytes=32 * 2**20
        ),
        name="yee",
    )(
        in_hbm(bloch_index),
        in_hbm(permittivity),
        absorption_peak,
        in_hbm(waveform),
        in_hbm(source_sheet),
        in_hbm(material),
        in_hbm(electric_in),
        in_hbm(magnetic_in),
    )
    return (electric_out, magnetic_out, reflected[:, :NSNAP], mean[0, :NSNAP])


def solution(mesh):
    in_specs = (
        P("ka", None),
        P("sp", None, None),
        P(),
        P(),
        P("ka", None, "sp", None),
        P(),
        P("ka", None, "sp", None, None),
        P("ka", None, "sp", None, None),
    )
    out_specs = (
        P("ka", None, "sp", None, None),
        P("ka", None, "sp", None, None),
        P("ka", None),
        P(),
    )
    return jax.shard_map(
        on_device, mesh=mesh, in_specs=in_specs, out_specs=out_specs, check_vma=False
    )
```

```python
import functools

import jax
import jax.numpy as jnp
from jax import lax
from jax.experimental import pallas as pl
from jax.experimental.pallas import tpu as pltpu
from jax.sharding import PartitionSpec as P

PML = 16
INTERVAL = 5
NSNAP = 2
MPHASE = 64
NMAT = 3
TIME_STEP = 0.5

MESH = pl.DeviceIdType.MESH
F32 = jnp.float32
TILE = 8


def kernel(
    sizes,
    bloch_in,
    permittivity_in,
    absorption_peak,
    waveform_in,
    sheet_in,
    material,
    e_in,
    h_in,
    e_out,
    h_out,
    sums_out,
    bloch,
    permittivity,
    waveform,
    ef,
    hf,
    e_low,
    h_low,
    mat,
    keep,
    gain,
    sheet_raw,
    sheet,
    from_up,
    from_down,
    ghost_h,
    ghost_ex,
    ghost_kind,
    ghost_raw,
    ghost_keep,
    ghost_gain,
    ghost_sheet,
    my_kind,
    totals,
    plane_sums,
    height_sums,
    load_sem,
    up_send,
    up_recv,
    down_send,
    down_recv,
    ghost_send,
    ghost_recv,
    extra_send,
    extra_recv,
    plane_send,
    plane_recv,
    height_send,
    height_recv,
    hello,
):
    points, slabs, rows, width, depth = sizes
    ka = lax.axis_index("ka")
    sp = lax.axis_index("sp")
    up = lax.rem(sp + 1, slabs)
    down = lax.rem(sp + slabs - 1, slabs)
    tiles = width // TILE
    last = rows - 1
    steps = NSNAP * INTERVAL
    heights = points // 4
    plane = 4 * slabs
    inside = pl.ds(TILE, width)
    whole = pl.ds(0, width)

    z_above_1 = lax.rem(ka + 4, points)
    z_below_1 = lax.rem(ka + points - 4, points)
    z_above_2 = lax.rem(ka + 8, points)
    z_below_2 = lax.rem(ka + points - 8, points)
    core_peer = ka + 1 - 2 * lax.rem(ka, 2)
    x_peer = ka + 2 - 4 * lax.rem(ka // 2, 2)

    barrier = pltpu.get_barrier_semaphore()
    near = [(ka, up), (ka, down)]
    near += [(peer, sp) for peer in (z_above_1, z_below_1, core_peer, x_peer)]
    for device in near:
        pl.semaphore_signal(barrier, inc=1, device_id=device, device_id_type=MESH)

    greetings = {
        0: ((), ((0, z_above_1), (1, z_below_1))),
        1: ((0, 1), ((2, z_above_2), (3, z_below_2))),
        2: ((2, 3), ()),
        5: ((), ((4, core_peer),)),
        6: ((4,), ((5, x_peer),)),
        7: ((5,), ()),
    }

    def exchange_greetings(index):
        waits, signals = greetings[index]
        for place in waits:
            pl.semaphore_wait(hello.at[place], 1)
        for place, peer in signals:
            pl.semaphore_signal(
                hello.at[place], inc=1, device_id=(peer, sp), device_id_type=MESH
            )

    def greet(step):
        for index in greetings:
            if index > 0:
                pl.when(step == index)(functools.partial(exchange_greetings, index))

    def load(source, target, index):
        copy = pltpu.make_async_copy(source, target, load_sem.at[index])
        copy.start()
        return copy

    middle = pl.ds(1, rows - 2)
    load_first = load(e_in.at[0, :, 0], e_low.at[:, 0], 0)
    load_last = load(e_in.at[0, :, last], e_low.at[:, last], 1)
    load_h_last = load(h_in.at[0, :, last], h_low.at[:, last], 2)
    load_mat_last = load(material.at[last], mat.at[last], 3)
    load_sheet = load(sheet_in.at[0], sheet_raw, 4)
    load_e = load(e_in.at[0, :, middle], e_low.at[:, middle], 5)
    load_h = load(h_in.at[0, :, pl.ds(0, last)], h_low.at[:, pl.ds(0, last)], 6)
    load_mat = load(material.at[pl.ds(0, last)], mat.at[pl.ds(0, last)], 7)
    small = [
        load(bloch_in, bloch, 8),
        load(permittivity_in, permittivity, 9),
        load(waveform_in, waveform, 10),
    ]

    def remote(source, target, send, recv, other):
        return pltpu.make_async_remote_copy(
            src_ref=source,
            dst_ref=target,
            send_sem=send,
            recv_sem=recv,
            device_id=(ka, other),
            device_id_type=MESH,
        )

    def copy_up(slot, chunk):
        where = pl.ds(chunk * TILE, TILE)
        return remote(
            ef.at[pl.ds(2, 4), last, where],
            from_down.at[slot, :, where],
            up_send.at[chunk],
            up_recv.at[slot, chunk],
            up,
        )

    def copy_down(slot, chunk):
        where = pl.ds(chunk * TILE, TILE)
        return remote(
            ef.at[pl.ds(2, 4), 0, where],
            from_up.at[slot, :, where],
            down_send.at[chunk],
            down_recv.at[slot, chunk],
            down,
        )

    def copy_ghost(chunk):
        where = pl.ds((chunk + 1) * TILE, TILE)
        return remote(
            hf.at[pl.ds(2, 4), last, where],
            ghost_h.at[:, where],
            ghost_send.at[chunk],
            ghost_recv.at[chunk],
            up,
        )

    extras = [
        remote(
            ef.at[pl.ds(0, 2), last, whole],
            ghost_ex.at[:, whole],
            extra_send.at[0],
            extra_recv.at[0],
            up,
        ),
        remote(my_kind, ghost_kind, extra_send.at[1], extra_recv.at[1], up),
        remote(
            sheet_raw.at[:, pl.ds(rows - TILE, TILE)],
            ghost_raw,
            extra_send.at[2],
            extra_recv.at[2],
            up,
        ),
    ]

    load_first.wait()
    for part in range(2, 6):
        ef[part, 0, whole, :] = e_low[part, 0].astype(F32)
    pl.semaphore_wait(barrier, len(near))
    for chunk in range(tiles):
        copy_down(0, chunk).start()
    load_last.wait()
    for part in range(6):
        ef[part, last, whole, :] = e_low[part, last].astype(F32)
    extras[0].start()
    load_mat_last.wait()
    my_kind[...] = mat[last].astype(F32)
    extras[1].start()
    load_sheet.wait()
    extras[2].start()
    load_h_last.wait()
    for part in range(6):
        hf[part, last, inside, :] = h_low[part, last].astype(F32)
    for part in range(2):
        ef[part, 0, whole, :] = e_low[part, 0].astype(F32)
    for copy in small:
        copy.wait()

    angle_x = jnp.full((1, depth), 2.0 * jnp.pi * bloch[0, 0].astype(F32) / MPHASE, F32)
    angle_y = jnp.full((1, depth), 2.0 * jnp.pi * bloch[0, 1].astype(F32) / MPHASE, F32)
    cos_x, sin_x = jnp.cos(angle_x), jnp.sin(angle_x)
    cos_y, sin_y = jnp.cos(angle_y), jnp.sin(angle_y)
    at_end = sp == slabs - 1
    at_start = sp == 0
    end_cos = jnp.where(at_end, cos_x, 1.0)
    end_sin = jnp.where(at_end, sin_x, 0.0)
    start_cos = jnp.where(at_start, cos_x, 1.0)
    start_sin = jnp.where(at_start, -sin_x, 0.0)

    lane = lax.broadcasted_iota(jnp.int32, (TILE, depth), 1)
    at_top = lane == depth - 1
    at_bottom = lane == 0

    def z_above(values):
        return jnp.where(at_top, 0.0, pltpu.roll(values, depth - 1, 1))

    def z_below(values):
        return jnp.where(at_bottom, 0.0, pltpu.roll(values, 1, 1))

    height = lane.astype(F32)
    low_depth = jnp.maximum(PML - height, 0.0) / PML
    high_depth = jnp.maximum(height - (depth - 1 - PML), 0.0) / PML
    conduct = absorption_peak[0] * (low_depth**3 + high_depth**3)
    half_mag = conduct * (0.5 * TIME_STEP)
    h_keep = (1.0 - half_mag) / (1.0 + half_mag)
    h_gain = -TIME_STEP / (1.0 + half_mag)

    def rotate(pair, cosine, sine):
        return (pair[0] * cosine - pair[1] * sine, pair[0] * sine + pair[1] * cosine)

    def upper_edge(refs):
        first, edge = pl.ds(0, 1), pl.ds(width, 1)
        real, imag = rotate((refs[0][first, :], refs[1][first, :]), cos_y, sin_y)
        refs[0][edge, :] = real
        refs[1][edge, :] = imag

    def lower_edge(refs):
        end, edge = pl.ds(width + TILE - 1, 1), pl.ds(TILE - 1, 1)
        real, imag = rotate((refs[0][end, :], refs[1][end, :]), cos_y, -sin_y)
        refs[0][edge, :] = real
        refs[1][edge, :] = imag

    def fill_e_edge(x):
        for part in (0, 4):
            upper_edge((ef.at[part, x], ef.at[part + 1, x]))

    def fill_h_edge(x, parts=(0, 4)):
        for part in parts:
            lower_edge((hf.at[part, x], hf.at[part + 1, x]))

    def fill_ghost_ex_edge():
        upper_edge((ghost_ex.at[0], ghost_ex.at[1]))

    def fill_ghost_h_edge():
        lower_edge((ghost_h.at[2], ghost_h.at[3]))

    keeps = []
    gains = []
    for level in range(NMAT):
        relative = jnp.full((TILE, depth), permittivity[level], F32)
        half_ele = conduct * (0.5 * TIME_STEP) / relative
        keeps.append((1.0 - half_ele) / (1.0 + half_ele))
        gains.append(TIME_STEP / relative / (1.0 + half_ele))

    def choose(kind, table, zero, one):
        return jnp.where(kind == zero, table[0], jnp.where(kind == one, table[1], table[2]))

    load_e.wait()
    load_h.wait()
    load_mat.wait()

    def widen_e(x, carry):
        for part in range(6):
            ef[part, x, whole, :] = e_low[part, x].astype(F32)
        fill_e_edge(x)
        return carry

    def widen_h(x, carry):
        for part in range(6):
            hf[part, x, inside, :] = h_low[part, x].astype(F32)
        return carry

    def fill_coefficients(x, carry):
        for tile in range(tiles):
            where = pl.ds(tile * TILE, TILE)
            kind = mat[x, where, :]
            keep[x, where, :] = choose(kind, keeps, 0, 1)
            gain[x, where, :] = choose(kind, gains, 0, 1)
        return carry

    fill_e_edge(0)
    fill_e_edge(last)
    lax.fori_loop(1, last, widen_e, 0)
    lax.fori_loop(0, last, widen_h, 0)
    lax.fori_loop(0, rows, fill_coefficients, 0)

    at_sheet = lax.broadcasted_iota(jnp.int32, (width, depth), 1) == PML + 2
    for part in range(2):
        turned = sheet_raw[part].T
        for x in range(rows):
            spread = jnp.broadcast_to(turned[:, x : x + 1], (width, depth))
            sheet[part, x] = jnp.where(at_sheet, spread, 0.0)

    def h_x(part, x, begin):
        ey = ef[2 + part, x, pl.ds(begin, TILE), :]
        ez = ef[4 + part, x, pl.ds(begin, TILE), :]
        ez_y = ef[4 + part, x, pl.ds(begin + 1, TILE), :]
        change = (ez_y - ez) - (z_above(ey) - ey)
        where = pl.ds(begin + TILE, TILE)
        hf[part, x, where, :] = h_keep * hf[part, x, where, :] + h_gain * change

    def h_yz(part, x, begin, ey_x, ez_x):
        ex = ef[part, x, pl.ds(begin, TILE), :]
        ex_y = ef[part, x, pl.ds(begin + 1, TILE), :]
        ey = ef[2 + part, x, pl.ds(begin, TILE), :]
        ez = ef[4 + part, x, pl.ds(begin, TILE), :]
        where = pl.ds(begin + TILE, TILE)
        change_y = (z_above(ex) - ex) - (ez_x - ez)
        change_z = (ey_x - ey) - (ex_y - ex)
        hf[2 + part, x, where, :] = h_keep * hf[2 + part, x, where, :] + h_gain * change_y
        hf[4 + part, x, where, :] = h_keep * hf[4 + part, x, where, :] + h_gain * change_z

    def ghost_h_yz(part, begin, ey, ez):
        ex = ghost_ex[part, pl.ds(begin, TILE), :]
        ex_y = ghost_ex[part, pl.ds(begin + 1, TILE), :]
        ey_x = ef[2 + part, 0, pl.ds(begin, TILE), :]
        ez_x = ef[4 + part, 0, pl.ds(begin, TILE), :]
        where = pl.ds(begin + TILE, TILE)
        change_y = (z_above(ex) - ex) - (ez_x - ez)
        change_z = (ey_x - ey) - (ex_y - ex)
        ghost_h[part, where, :] = h_keep * ghost_h[part, where, :] + h_gain * change_y
        ghost_h[2 + part, where, :] = h_keep * ghost_h[2 + part, where, :] + h_gain * change_z

    def e_x(part, x, begin, drive):
        where = pl.ds(begin, TILE)
        hy = hf[2 + part, x, pl.ds(begin + TILE, TILE), :]
        hz = hf[4 + part, x, pl.ds(begin + TILE, TILE), :]
        hz_y = hf[4 + part, x, pl.ds(begin + TILE - 1, TILE), :]
        change = (hz - hz_y) - (hy - z_below(hy)) - drive * sheet[part, x, where, :]
        ef[part, x, where, :] = (
            keep[x, where, :] * ef[part, x, where, :] + gain[x, where, :] * change
        )

    def ghost_e_x(part, begin, drive):
        where = pl.ds(begin, TILE)
        hy = ghost_h[part, pl.ds(begin + TILE, TILE), :]
        hz = ghost_h[2 + part, pl.ds(begin + TILE, TILE), :]
        hz_y = ghost_h[2 + part, pl.ds(begin + TILE - 1, TILE), :]
        change = (hz - hz_y) - (hy - z_below(hy)) - drive * ghost_sheet[part, where, :]
        ghost_ex[part, where, :] = (
            ghost_keep[where, :] * ghost_ex[part, where, :] + ghost_gain[where, :] * change
        )

    def e_yz(part, x, begin, hy_x, hz_x):
        where = pl.ds(begin, TILE)
        hx = hf[part, x, pl.ds(begin + TILE, TILE), :]
        hx_y = hf[part, x, pl.ds(begin + TILE - 1, TILE), :]
        hy = hf[2 + part, x, pl.ds(begin + TILE, TILE), :]
        hz = hf[4 + part, x, pl.ds(begin + TILE, TILE), :]
        change_y = (hx - z_below(hx)) - (hz - hz_x)
        change_z = (hy - hy_x) - (hx - hx_y)
        retain = keep[x, where, :]
        factor = gain[x, where, :]
        ef[2 + part, x, where, :] = retain * ef[2 + part, x, where, :] + factor * change_y
        ef[4 + part, x, where, :] = retain * ef[4 + part, x, where, :] + factor * change_z

    def h_row(x, carry):
        for tile in range(tiles):
            begin = tile * TILE
            where = pl.ds(begin, TILE)
            for part in range(2):
                h_x(part, x, begin)
                h_yz(
                    part, x, begin, ef[2 + part, x + 1, where, :], ef[4 + part, x + 1, where, :]
                )
        fill_h_edge(x)
        return carry

    def h_row_out(x, carry):
        h_row(x, carry)
        for part in range(6):
            h_out[0, part, x] = hf[part, x, inside, :]
        return carry

    def e_row(drive, x, carry):
        for tile in range(tiles):
            begin = tile * TILE
            where = pl.ds(begin + TILE, TILE)
            for part in range(2):
                e_x(part, x, begin, drive)
                e_yz(
                    part, x, begin, hf[2 + part, x - 1, where, :], hf[4 + part, x - 1, where, :]
                )
        fill_e_edge(x)
        return carry

    def add_power(index, x):
        total = totals[index]
        for part in range(4):
            for tile in range(tiles):
                values = ef[part, x, pl.ds(tile * TILE, TILE), :]
                total = total + values * values
        totals[index] = total

    def e_row_out(drive, x, carry):
        e_row(drive, x, carry)
        for part in range(6):
            e_out[0, part, x] = ef[part, x, whole, :]
        add_power(NSNAP - 1, x)
        return carry

    def e_x_ends(drive):
        for x in (0, last):
            for tile in range(tiles):
                for part in range(2):
                    e_x(part, x, tile * TILE, drive)

    def finish_electric(drive):
        fill_h_edge(last, (4,))
        fill_ghost_h_edge()
        for tile in range(tiles):
            for part in range(2):
                ghost_e_x(part, tile * TILE, drive)
        fill_ghost_ex_edge()
        e_x_ends(drive)
        fill_e_edge(0)
        fill_e_edge(last)
        e_row(drive, 1, 0)
        e_row(drive, last - 1, 0)

    def begin_magnetic():
        h_row(0, 0)
        h_row(last - 1, 0)
        for tile in range(tiles):
            for part in range(2):
                h_x(part, last, tile * TILE)
        fill_h_edge(last, (0,))

    def pair_of(ref, part, where):
        return (ref[part, where, :], ref[part + 1, where, :])

    def receive(slot, chunk):
        arriving_up = copy_up(slot, chunk)
        arriving_down = copy_down(slot, chunk)
        arriving_up.wait()
        arriving_down.wait()
        begin = chunk * TILE
        where = pl.ds(begin, TILE)
        ey_up = rotate(pair_of(from_up.at[slot], 0, where), end_cos, end_sin)
        ez_up = rotate(pair_of(from_up.at[slot], 2, where), end_cos, end_sin)
        ey_down = rotate(pair_of(from_down.at[slot], 0, where), start_cos, start_sin)
        ez_down = rotate(pair_of(from_down.at[slot], 2, where), start_cos, start_sin)
        beyond = pl.ds(begin + TILE, TILE)
        for part in range(2):
            h_yz(part, last, begin, ey_up[part], ez_up[part])
            ghost_h_yz(part, begin, ey_down[part], ez_down[part])
        for part in range(2):
            e_yz(part, last, begin, hf[2 + part, last - 1, beyond, :], hf[4 + part, last - 1, beyond, :])
            e_yz(part, 0, begin, ghost_h[part, beyond, :], ghost_h[2 + part, beyond, :])

    def share(first, end, part, pieces):
        count = end - first
        return first + count * part // pieces, first + count * (part + 1) // pieces

    totals[...] = jnp.zeros(totals.shape, F32)

    def finish_ghost():
        for extra in extras:
            extra.wait()
        real, imag = rotate((ghost_ex[0, whole, :], ghost_ex[1, whole, :]), start_cos, start_sin)
        ghost_ex[0, whole, :] = real
        ghost_ex[1, whole, :] = imag
        for tile in range(tiles):
            where = pl.ds(tile * TILE, TILE)
            kind = ghost_kind[where, :]
            ghost_keep[where, :] = choose(kind, keeps, 0.0, 1.0)
            ghost_gain[where, :] = choose(kind, gains, 0.0, 1.0)
        real, imag = rotate(
            (ghost_raw[0], ghost_raw[1]), start_cos[:, :width], start_sin[:, :width]
        )
        for part, raw in enumerate((real, imag)):
            column = raw.T[:, TILE - 1 : TILE]
            spread = jnp.broadcast_to(column, (width, depth))
            ghost_sheet[part] = jnp.where(at_sheet, spread, 0.0)

    half = tiles // 2

    def between(first, end, part, pieces, row):
        begin, end = share(first, end, part, pieces)
        lax.fori_loop(begin, end, row, 0)

    begin_magnetic()
    exchange_greetings(0)
    for chunk in range(tiles):
        copy_down(0, chunk).wait()
        begin = chunk * TILE
        where = pl.ds(begin, TILE)
        beyond = pl.ds(begin + TILE, TILE)
        ey_up = rotate(pair_of(from_up.at[0], 0, where), end_cos, end_sin)
        ez_up = rotate(pair_of(from_up.at[0], 2, where), end_cos, end_sin)
        for part in range(2):
            h_yz(part, last, begin, ey_up[part], ez_up[part])
        copy_ghost(chunk).start()
        for part in range(2):
            e_yz(
                part, last, begin, hf[2 + part, last - 1, beyond, :], hf[4 + part, last - 1, beyond, :]
            )
        copy_up(1, chunk).start()
        between(1, last - 1, chunk, tiles, h_row)
    for chunk in range(tiles):
        copy_ghost(chunk).wait()
        begin = chunk * TILE
        beyond = pl.ds(begin + TILE, TILE)
        for part in (0, 2):
            real, imag = rotate(pair_of(ghost_h, part, beyond), start_cos, start_sin)
            ghost_h[part, beyond, :] = real
            ghost_h[part + 1, beyond, :] = imag
        for part in range(2):
            e_yz(part, 0, begin, ghost_h[part, beyond, :], ghost_h[2 + part, beyond, :])
        copy_down(1, chunk).start()
    finish_ghost()

    def advance(step, carry):
        slot = lax.rem(step, 2)
        drive = waveform[step - 1]
        finish_electric(drive)

        @pl.when(step == INTERVAL)
        def _():
            for x in (0, 1, last - 1, last):
                add_power(0, x)

        begin_magnetic()
        greet(step)
        for chunk in range(tiles):
            receive(slot, chunk)
            copy_up(1 - slot, chunk).start()
            copy_down(1 - slot, chunk).start()
            if chunk < half:
                between(2, last - 1, chunk, half, functools.partial(e_row, drive))
            else:
                between(1, last - 1, chunk - half, tiles - half, h_row)

        @pl.when(step == INTERVAL)
        def _():
            def add(x, inner):
                add_power(0, x)
                return inner

            lax.fori_loop(2, last - 1, add, 0)

        return carry

    lax.fori_loop(1, steps - 1, advance, 0)

    slot = (steps - 1) % 2
    drive = waveform[steps - 2]
    finish_electric(drive)
    lax.fori_loop(2, last - 1, functools.partial(e_row, drive), 0)
    begin_magnetic()
    lax.fori_loop(1, last - 1, h_row_out, 0)
    for x in (0, last - 1):
        for part in range(6):
            h_out[0, part, x] = hf[part, x, inside, :]
    final = waveform[steps - 1]
    lax.fori_loop(1, last, functools.partial(e_row_out, final), 0)
    for chunk in range(tiles):
        receive(slot, chunk)
    fill_h_edge(last, (4,))
    e_x_ends(final)
    add_power(NSNAP - 1, 0)
    add_power(NSNAP - 1, last)

    at_row = lax.broadcasted_iota(jnp.int32, (1, depth), 1)
    mine = jnp.zeros((1, depth), F32)
    for snap in range(NSNAP):
        power = jnp.sum(totals[snap], axis=0, keepdims=True)
        moved = pltpu.roll(power, depth - (PML + 6) + snap, 1)
        mine = jnp.where(at_row == snap, moved, mine)
    plane_sums[0] = mine

    group = points // heights
    place = lax.rem(ka, group)

    def plane_copy(index):
        offset = lax.rem(index + plane // 2, plane - 1) + 1
        peer = ka - place + lax.rem(place + offset // slabs, group)
        return pltpu.make_async_remote_copy(
            src_ref=plane_sums.at[0],
            dst_ref=plane_sums.at[offset],
            send_sem=plane_send.at[offset],
            recv_sem=plane_recv.at[offset],
            device_id=(peer, lax.rem(sp + lax.rem(offset, slabs), slabs)),
            device_id_type=MESH,
        )

    def height_copy(index):
        offset = lax.rem(index + heights // 2 - 1, heights - 1) + 1
        return pltpu.make_async_remote_copy(
            src_ref=height_sums.at[0],
            dst_ref=height_sums.at[offset],
            send_sem=height_send.at[offset],
            recv_sem=height_recv.at[offset],
            device_id=(lax.rem(ka + group * offset, points), sp),
            device_id_type=MESH,
        )

    def started(copy):
        def start(index, carry):
            copy(index).start()
            return carry

        return start

    def waited(copy):
        def wait(index, carry):
            copy(index).wait()
            return carry

        return wait

    lax.fori_loop(0, plane - 1, started(plane_copy), 0)
    for x in (0, last):
        for part in range(6):
            e_out[0, part, x] = ef[part, x, whole, :]
    for part in range(6):
        h_out[0, part, last] = hf[part, last, inside, :]
    lax.fori_loop(0, plane - 1, waited(plane_copy), 0)
    slab_total = plane_sums[0]
    for offset in range(1, slabs):
        slab_total = slab_total + plane_sums[offset]
    total = slab_total
    for offset in range(slabs, plane):
        total = total + plane_sums[offset]
    height_sums[0] = total
    lax.fori_loop(0, heights - 1, started(height_copy), 0)
    cells = rows * slabs * width
    sums_out[pl.ds(0, 1), :] = slab_total / cells
    lax.fori_loop(0, heights - 1, waited(height_copy), 0)
    total = height_sums[0]
    for offset in range(1, heights):
        total = total + height_sums[offset]
    sums_out[pl.ds(1, 1), :] = total / cells / points


def in_hbm(values):
    return pltpu.with_memory_space_constraint(values, pltpu.HBM)


def on_device(
    bloch_index,
    material,
    permittivity,
    absorption_peak,
    source_sheet,
    waveform,
    electric_in,
    magnetic_in,
):
    rows, width, depth = material.shape
    slabs = lax.axis_size("sp")
    points = lax.axis_size("ka")
    tiles = width // TILE
    vmem = pl.BlockSpec(memory_space=pltpu.VMEM)
    hbm = pl.BlockSpec(memory_space=pltpu.HBM)
    dma = pltpu.SemaphoreType.DMA
    electric_out, magnetic_out, sums = pl.pallas_call(
        functools.partial(kernel, (points, slabs, rows, width, depth)),
        out_shape=(
            jax.ShapeDtypeStruct(electric_in.shape, F32),
            jax.ShapeDtypeStruct(magnetic_in.shape, F32),
            jax.ShapeDtypeStruct((2, depth), F32),
        ),
        in_specs=[hbm, hbm, pl.BlockSpec(memory_space=pltpu.SMEM)] + [hbm] * 5,
        out_specs=(vmem, vmem, vmem),
        scratch_shapes=[
            pltpu.SMEM(bloch_index.shape, jnp.int32),
            pltpu.SMEM(permittivity.shape, F32),
            pltpu.SMEM(waveform.shape, F32),
            pltpu.VMEM((6, rows, width + TILE, depth), F32),
            pltpu.VMEM((6, rows, width + TILE, depth), F32),
            pltpu.VMEM((6, rows, width, depth), jnp.bfloat16),
            pltpu.VMEM((6, rows, width, depth), jnp.bfloat16),
            pltpu.VMEM((rows, width, depth), jnp.int32),
            pltpu.VMEM((rows, width, depth), F32),
            pltpu.VMEM((rows, width, depth), F32),
            pltpu.VMEM((2, rows, width), F32),
            pltpu.VMEM((2, rows, width, depth), F32),
            pltpu.VMEM((2, 4, width, depth), F32),
            pltpu.VMEM((2, 4, width, depth), F32),
            pltpu.VMEM((4, width + TILE, depth), F32),
            pltpu.VMEM((2, width + TILE, depth), F32),
            pltpu.VMEM((width, depth), F32),
            pltpu.VMEM((2, TILE, width), F32),
            pltpu.VMEM((width, depth), F32),
            pltpu.VMEM((width, depth), F32),
            pltpu.VMEM((2, width, depth), F32),
            pltpu.VMEM((width, depth), F32),
            pltpu.VMEM((NSNAP, TILE, depth), F32),
            pltpu.VMEM((4 * slabs, 1, depth), F32),
            pltpu.VMEM((points // 4, 1, depth), F32),
            dma((11,)),
            dma((tiles,)),
            dma((2, tiles)),
            dma((tiles,)),
            dma((2, tiles)),
            dma((tiles,)),
            dma((tiles,)),
            dma((3,)),
            dma((3,)),
            dma((4 * slabs,)),
            dma((4 * slabs,)),
            dma((points // 4,)),
            dma((points // 4,)),
            pltpu.SemaphoreType.REGULAR((6,)),
        ],
        compiler_params=pltpu.CompilerParams(
            collective_id=0, has_side_effects=True, vmem_limit_bytes=32 * 2**20
        ),
        name="yee",
    )(
        in_hbm(bloch_index),
        in_hbm(permittivity),
        absorption_peak,
        in_hbm(waveform),
        in_hbm(source_sheet),
        in_hbm(material),
        in_hbm(electric_in),
        in_hbm(magnetic_in),
    )
    return (electric_out, magnetic_out, sums[:1, :NSNAP], sums[1, :NSNAP])


def solution(mesh):
    in_specs = (
        P("ka", None),
        P("sp", None, None),
        P(),
        P(),
        P("ka", None, "sp", None),
        P(),
        P("ka", None, "sp", None, None),
        P("ka", None, "sp", None, None),
    )
    out_specs = (
        P("ka", None, "sp", None, None),
        P("ka", None, "sp", None, None),
        P("ka", None),
        P(),
    )
    return jax.shard_map(
        on_device, mesh=mesh, in_specs=in_specs, out_specs=out_specs, check_vma=False
    )
```

```python
import functools

import jax
import jax.numpy as jnp
from jax import lax
from jax.experimental import pallas as pl
from jax.experimental.pallas import tpu as pltpu
from jax.sharding import PartitionSpec as P

PML = 16
INTERVAL = 5
NSNAP = 2
MPHASE = 64
NMAT = 3
TIME_STEP = 0.5

MESH = pl.DeviceIdType.MESH
F32 = jnp.float32
TILE = 8


def kernel(
    sizes,
    bloch_in,
    permittivity_in,
    absorption_peak,
    waveform_in,
    sheet_in,
    material,
    e_in,
    h_in,
    e_out,
    h_out,
    sums_out,
    bloch,
    permittivity,
    waveform,
    ef,
    hf,
    e_low,
    h_low,
    mat,
    keep,
    gain,
    sheet_raw,
    sheet,
    from_up,
    from_down,
    ghost_h,
    ghost_ex,
    ghost_kind,
    ghost_raw,
    ghost_keep,
    ghost_gain,
    ghost_sheet,
    my_kind,
    totals,
    plane_sums,
    height_sums,
    load_sem,
    up_send,
    up_recv,
    down_send,
    down_recv,
    ghost_send,
    ghost_recv,
    extra_send,
    extra_recv,
    plane_send,
    plane_recv,
    height_send,
    height_recv,
    hello,
    pace,
):
    points, slabs, rows, width, depth = sizes
    ka = lax.axis_index("ka")
    sp = lax.axis_index("sp")
    up = lax.rem(sp + 1, slabs)
    down = lax.rem(sp + slabs - 1, slabs)
    tiles = width // TILE
    last = rows - 1
    steps = NSNAP * INTERVAL
    heights = points // 4
    plane = 4 * slabs
    inside = pl.ds(TILE, width)
    whole = pl.ds(0, width)

    z_above_1 = lax.rem(ka + 4, points)
    z_below_1 = lax.rem(ka + points - 4, points)
    z_above_2 = lax.rem(ka + 8, points)
    z_below_2 = lax.rem(ka + points - 8, points)
    core_peer = ka + 1 - 2 * lax.rem(ka, 2)
    x_peer = ka + 2 - 4 * lax.rem(ka // 2, 2)

    barrier = pltpu.get_barrier_semaphore()
    near = [(ka, up), (ka, down)]
    near += [(peer, sp) for peer in (z_above_1, z_below_1, core_peer, x_peer)]
    for device in near:
        pl.semaphore_signal(barrier, inc=1, device_id=device, device_id_type=MESH)

    greetings = {
        0: ((), ((0, z_above_1), (1, z_below_1))),
        1: ((0, 1), ((2, z_above_2), (3, z_below_2))),
        2: ((2, 3), ()),
        5: ((), ((4, core_peer),)),
        6: ((4,), ((5, x_peer),)),
        7: ((5,), ()),
    }

    def exchange_greetings(index):
        waits, signals = greetings[index]
        for place in waits:
            pl.semaphore_wait(hello.at[place], 1)
        for place, peer in signals:
            pl.semaphore_signal(
                hello.at[place], inc=1, device_id=(peer, sp), device_id_type=MESH
            )

    def greet(step):
        for index in greetings:
            if index > 0:
                pl.when(step == index)(functools.partial(exchange_greetings, index))

    def load(source, target, index):
        copy = pltpu.make_async_copy(source, target, load_sem.at[index])
        copy.start()
        return copy

    middle = pl.ds(1, rows - 2)
    load_first = load(e_in.at[0, :, 0], e_low.at[:, 0], 0)
    load_last = load(e_in.at[0, :, last], e_low.at[:, last], 1)
    load_h_last = load(h_in.at[0, :, last], h_low.at[:, last], 2)
    load_mat_last = load(material.at[last], mat.at[last], 3)
    load_sheet = load(sheet_in.at[0], sheet_raw, 4)
    load_e = load(e_in.at[0, :, middle], e_low.at[:, middle], 5)
    load_h = load(h_in.at[0, :, pl.ds(0, last)], h_low.at[:, pl.ds(0, last)], 6)
    load_mat = load(material.at[pl.ds(0, last)], mat.at[pl.ds(0, last)], 7)
    small = [
        load(bloch_in, bloch, 8),
        load(permittivity_in, permittivity, 9),
        load(waveform_in, waveform, 10),
    ]

    def remote(source, target, send, recv, other):
        return pltpu.make_async_remote_copy(
            src_ref=source,
            dst_ref=target,
            send_sem=send,
            recv_sem=recv,
            device_id=(ka, other),
            device_id_type=MESH,
        )

    def copy_up(slot, chunk):
        where = pl.ds(chunk * TILE, TILE)
        return remote(
            ef.at[pl.ds(2, 4), last, where],
            from_down.at[slot, :, where],
            up_send.at[chunk],
            up_recv.at[slot, chunk],
            up,
        )

    def copy_down(slot, chunk):
        where = pl.ds(chunk * TILE, TILE)
        return remote(
            ef.at[pl.ds(2, 4), 0, where],
            from_up.at[slot, :, where],
            down_send.at[chunk],
            down_recv.at[slot, chunk],
            down,
        )

    def copy_ghost(chunk):
        where = pl.ds((chunk + 1) * TILE, TILE)
        return remote(
            hf.at[pl.ds(2, 4), last, where],
            ghost_h.at[:, where],
            ghost_send.at[chunk],
            ghost_recv.at[chunk],
            up,
        )

    extras = [
        remote(
            ef.at[pl.ds(0, 2), last, whole],
            ghost_ex.at[:, whole],
            extra_send.at[0],
            extra_recv.at[0],
            up,
        ),
        remote(my_kind, ghost_kind, extra_send.at[1], extra_recv.at[1], up),
        remote(
            sheet_raw.at[:, pl.ds(rows - TILE, TILE)],
            ghost_raw,
            extra_send.at[2],
            extra_recv.at[2],
            up,
        ),
    ]

    load_first.wait()
    for part in range(2, 6):
        ef[part, 0, whole, :] = e_low[part, 0].astype(F32)
    pl.semaphore_wait(barrier, len(near))
    for chunk in range(tiles):
        copy_down(0, chunk).start()
    load_last.wait()
    for part in range(6):
        ef[part, last, whole, :] = e_low[part, last].astype(F32)
    extras[0].start()
    load_mat_last.wait()
    my_kind[...] = mat[last].astype(F32)
    extras[1].start()
    load_sheet.wait()
    extras[2].start()
    load_h_last.wait()
    for part in range(6):
        hf[part, last, inside, :] = h_low[part, last].astype(F32)
    for part in range(2):
        ef[part, 0, whole, :] = e_low[part, 0].astype(F32)
    for copy in small:
        copy.wait()

    angle_x = jnp.full((1, depth), 2.0 * jnp.pi * bloch[0, 0].astype(F32) / MPHASE, F32)
    angle_y = jnp.full((1, depth), 2.0 * jnp.pi * bloch[0, 1].astype(F32) / MPHASE, F32)
    cos_x, sin_x = jnp.cos(angle_x), jnp.sin(angle_x)
    cos_y, sin_y = jnp.cos(angle_y), jnp.sin(angle_y)
    at_end = sp == slabs - 1
    at_start = sp == 0
    end_cos = jnp.where(at_end, cos_x, 1.0)
    end_sin = jnp.where(at_end, sin_x, 0.0)
    start_cos = jnp.where(at_start, cos_x, 1.0)
    start_sin = jnp.where(at_start, -sin_x, 0.0)

    lane = lax.broadcasted_iota(jnp.int32, (TILE, depth), 1)
    at_top = lane == depth - 1
    at_bottom = lane == 0

    def z_above(values):
        return jnp.where(at_top, 0.0, pltpu.roll(values, depth - 1, 1))

    def z_below(values):
        return jnp.where(at_bottom, 0.0, pltpu.roll(values, 1, 1))

    height = lane.astype(F32)
    low_depth = jnp.maximum(PML - height, 0.0) / PML
    high_depth = jnp.maximum(height - (depth - 1 - PML), 0.0) / PML
    conduct = absorption_peak[0] * (low_depth**3 + high_depth**3)
    half_mag = conduct * (0.5 * TIME_STEP)
    h_keep = (1.0 - half_mag) / (1.0 + half_mag)
    h_gain = -TIME_STEP / (1.0 + half_mag)

    def rotate(pair, cosine, sine):
        return (pair[0] * cosine - pair[1] * sine, pair[0] * sine + pair[1] * cosine)

    def upper_edge(refs):
        first, edge = pl.ds(0, 1), pl.ds(width, 1)
        real, imag = rotate((refs[0][first, :], refs[1][first, :]), cos_y, sin_y)
        refs[0][edge, :] = real
        refs[1][edge, :] = imag

    def lower_edge(refs):
        end, edge = pl.ds(width + TILE - 1, 1), pl.ds(TILE - 1, 1)
        real, imag = rotate((refs[0][end, :], refs[1][end, :]), cos_y, -sin_y)
        refs[0][edge, :] = real
        refs[1][edge, :] = imag

    def fill_e_edge(x):
        for part in (0, 4):
            upper_edge((ef.at[part, x], ef.at[part + 1, x]))

    def fill_h_edge(x, parts=(0, 4)):
        for part in parts:
            lower_edge((hf.at[part, x], hf.at[part + 1, x]))

    def fill_ghost_ex_edge():
        upper_edge((ghost_ex.at[0], ghost_ex.at[1]))

    def fill_ghost_h_edge():
        lower_edge((ghost_h.at[2], ghost_h.at[3]))

    keeps = []
    gains = []
    for level in range(NMAT):
        relative = jnp.full((TILE, depth), permittivity[level], F32)
        half_ele = conduct * (0.5 * TIME_STEP) / relative
        keeps.append((1.0 - half_ele) / (1.0 + half_ele))
        gains.append(TIME_STEP / relative / (1.0 + half_ele))

    def choose(kind, table, zero, one):
        return jnp.where(kind == zero, table[0], jnp.where(kind == one, table[1], table[2]))

    load_e.wait()
    load_h.wait()
    load_mat.wait()

    def widen_e(x, carry):
        for part in range(6):
            ef[part, x, whole, :] = e_low[part, x].astype(F32)
        fill_e_edge(x)
        return carry

    def widen_h(x, carry):
        for part in range(6):
            hf[part, x, inside, :] = h_low[part, x].astype(F32)
        return carry

    def fill_coefficients(x, carry):
        for tile in range(tiles):
            where = pl.ds(tile * TILE, TILE)
            kind = mat[x, where, :]
            keep[x, where, :] = choose(kind, keeps, 0, 1)
            gain[x, where, :] = choose(kind, gains, 0, 1)
        return carry

    fill_e_edge(0)
    fill_e_edge(last)
    lax.fori_loop(1, last, widen_e, 0)
    lax.fori_loop(0, last, widen_h, 0)
    lax.fori_loop(0, rows, fill_coefficients, 0)

    at_sheet = lax.broadcasted_iota(jnp.int32, (width, depth), 1) == PML + 2
    for part in range(2):
        turned = sheet_raw[part].T
        for x in range(rows):
            spread = jnp.broadcast_to(turned[:, x : x + 1], (width, depth))
            sheet[part, x] = jnp.where(at_sheet, spread, 0.0)

    def h_x(part, x, begin):
        ey = ef[2 + part, x, pl.ds(begin, TILE), :]
        ez = ef[4 + part, x, pl.ds(begin, TILE), :]
        ez_y = ef[4 + part, x, pl.ds(begin + 1, TILE), :]
        change = (ez_y - ez) - (z_above(ey) - ey)
        where = pl.ds(begin + TILE, TILE)
        hf[part, x, where, :] = h_keep * hf[part, x, where, :] + h_gain * change

    def h_yz(part, x, begin, ey_x, ez_x):
        ex = ef[part, x, pl.ds(begin, TILE), :]
        ex_y = ef[part, x, pl.ds(begin + 1, TILE), :]
        ey = ef[2 + part, x, pl.ds(begin, TILE), :]
        ez = ef[4 + part, x, pl.ds(begin, TILE), :]
        where = pl.ds(begin + TILE, TILE)
        change_y = (z_above(ex) - ex) - (ez_x - ez)
        change_z = (ey_x - ey) - (ex_y - ex)
        hf[2 + part, x, where, :] = h_keep * hf[2 + part, x, where, :] + h_gain * change_y
        hf[4 + part, x, where, :] = h_keep * hf[4 + part, x, where, :] + h_gain * change_z

    def ghost_h_yz(part, begin, ey, ez):
        ex = ghost_ex[part, pl.ds(begin, TILE), :]
        ex_y = ghost_ex[part, pl.ds(begin + 1, TILE), :]
        ey_x = ef[2 + part, 0, pl.ds(begin, TILE), :]
        ez_x = ef[4 + part, 0, pl.ds(begin, TILE), :]
        where = pl.ds(begin + TILE, TILE)
        change_y = (z_above(ex) - ex) - (ez_x - ez)
        change_z = (ey_x - ey) - (ex_y - ex)
        ghost_h[part, where, :] = h_keep * ghost_h[part, where, :] + h_gain * change_y
        ghost_h[2 + part, where, :] = h_keep * ghost_h[2 + part, where, :] + h_gain * change_z

    def e_x(part, x, begin, drive):
        where = pl.ds(begin, TILE)
        hy = hf[2 + part, x, pl.ds(begin + TILE, TILE), :]
        hz = hf[4 + part, x, pl.ds(begin + TILE, TILE), :]
        hz_y = hf[4 + part, x, pl.ds(begin + TILE - 1, TILE), :]
        change = (hz - hz_y) - (hy - z_below(hy)) - drive * sheet[part, x, where, :]
        ef[part, x, where, :] = (
            keep[x, where, :] * ef[part, x, where, :] + gain[x, where, :] * change
        )

    def ghost_e_x(part, begin, drive):
        where = pl.ds(begin, TILE)
        hy = ghost_h[part, pl.ds(begin + TILE, TILE), :]
        hz = ghost_h[2 + part, pl.ds(begin + TILE, TILE), :]
        hz_y = ghost_h[2 + part, pl.ds(begin + TILE - 1, TILE), :]
        change = (hz - hz_y) - (hy - z_below(hy)) - drive * ghost_sheet[part, where, :]
        ghost_ex[part, where, :] = (
            ghost_keep[where, :] * ghost_ex[part, where, :] + ghost_gain[where, :] * change
        )

    def e_yz(part, x, begin, hy_x, hz_x):
        where = pl.ds(begin, TILE)
        hx = hf[part, x, pl.ds(begin + TILE, TILE), :]
        hx_y = hf[part, x, pl.ds(begin + TILE - 1, TILE), :]
        hy = hf[2 + part, x, pl.ds(begin + TILE, TILE), :]
        hz = hf[4 + part, x, pl.ds(begin + TILE, TILE), :]
        change_y = (hx - z_below(hx)) - (hz - hz_x)
        change_z = (hy - hy_x) - (hx - hx_y)
        retain = keep[x, where, :]
        factor = gain[x, where, :]
        ef[2 + part, x, where, :] = retain * ef[2 + part, x, where, :] + factor * change_y
        ef[4 + part, x, where, :] = retain * ef[4 + part, x, where, :] + factor * change_z

    def h_row(x, carry):
        for tile in range(tiles):
            begin = tile * TILE
            where = pl.ds(begin, TILE)
            for part in range(2):
                h_x(part, x, begin)
                h_yz(
                    part, x, begin, ef[2 + part, x + 1, where, :], ef[4 + part, x + 1, where, :]
                )
        fill_h_edge(x)
        return carry

    def h_row_out(x, carry):
        h_row(x, carry)
        for part in range(6):
            h_out[0, part, x] = hf[part, x, inside, :]
        return carry

    def e_row(drive, x, carry):
        for tile in range(tiles):
            begin = tile * TILE
            where = pl.ds(begin + TILE, TILE)
            for part in range(2):
                e_x(part, x, begin, drive)
                e_yz(
                    part, x, begin, hf[2 + part, x - 1, where, :], hf[4 + part, x - 1, where, :]
                )
        fill_e_edge(x)
        return carry

    def add_power(index, x):
        total = totals[index]
        for part in range(4):
            for tile in range(tiles):
                values = ef[part, x, pl.ds(tile * TILE, TILE), :]
                total = total + values * values
        totals[index] = total

    def e_row_out(drive, x, carry):
        e_row(drive, x, carry)
        for part in range(6):
            e_out[0, part, x] = ef[part, x, whole, :]
        add_power(NSNAP - 1, x)
        return carry

    def e_x_plane(x, drive):
        for tile in range(tiles):
            for part in range(2):
                e_x(part, x, tile * TILE, drive)

    def finish_electric(drive):
        fill_h_edge(last, (4,))
        fill_ghost_h_edge()
        for tile in range(tiles):
            for part in range(2):
                ghost_e_x(part, tile * TILE, drive)
        fill_ghost_ex_edge()
        e_x_plane(0, drive)
        e_x_plane(last, drive)
        fill_e_edge(0)
        fill_e_edge(last)
        e_row(drive, 1, 0)
        e_row(drive, last - 1, 0)

    def begin_magnetic():
        h_row(0, 0)
        h_row(last - 1, 0)
        for tile in range(tiles):
            for part in range(2):
                h_x(part, last, tile * TILE)
        fill_h_edge(last, (0,))

    def pair_of(ref, part, where):
        return (ref[part, where, :], ref[part + 1, where, :])

    def receive(slot, chunk):
        arriving_up = copy_up(slot, chunk)
        arriving_down = copy_down(slot, chunk)
        arriving_up.wait()
        arriving_down.wait()
        begin = chunk * TILE
        where = pl.ds(begin, TILE)
        ey_up = rotate(pair_of(from_up.at[slot], 0, where), end_cos, end_sin)
        ez_up = rotate(pair_of(from_up.at[slot], 2, where), end_cos, end_sin)
        ey_down = rotate(pair_of(from_down.at[slot], 0, where), start_cos, start_sin)
        ez_down = rotate(pair_of(from_down.at[slot], 2, where), start_cos, start_sin)
        beyond = pl.ds(begin + TILE, TILE)
        for part in range(2):
            h_yz(part, last, begin, ey_up[part], ez_up[part])
            ghost_h_yz(part, begin, ey_down[part], ez_down[part])
        for part in range(2):
            e_yz(part, last, begin, hf[2 + part, last - 1, beyond, :], hf[4 + part, last - 1, beyond, :])
            e_yz(part, 0, begin, ghost_h[part, beyond, :], ghost_h[2 + part, beyond, :])

    def share(first, end, part, pieces):
        count = end - first
        return first + count * part // pieces, first + count * (part + 1) // pieces

    totals[...] = jnp.zeros(totals.shape, F32)

    def finish_ghost():
        for extra in extras:
            extra.wait()
        real, imag = rotate((ghost_ex[0, whole, :], ghost_ex[1, whole, :]), start_cos, start_sin)
        ghost_ex[0, whole, :] = real
        ghost_ex[1, whole, :] = imag
        for tile in range(tiles):
            where = pl.ds(tile * TILE, TILE)
            kind = ghost_kind[where, :]
            ghost_keep[where, :] = choose(kind, keeps, 0.0, 1.0)
            ghost_gain[where, :] = choose(kind, gains, 0.0, 1.0)
        real, imag = rotate(
            (ghost_raw[0], ghost_raw[1]), start_cos[:, :width], start_sin[:, :width]
        )
        for part, raw in enumerate((real, imag)):
            column = raw.T[:, TILE - 1 : TILE]
            spread = jnp.broadcast_to(column, (width, depth))
            ghost_sheet[part] = jnp.where(at_sheet, spread, 0.0)

    half = tiles // 2

    def between(first, end, part, pieces, row):
        begin, end = share(first, end, part, pieces)
        lax.fori_loop(begin, end, row, 0)

    begin_magnetic()
    exchange_greetings(0)
    for chunk in range(tiles):
        copy_down(0, chunk).wait()
        begin = chunk * TILE
        where = pl.ds(begin, TILE)
        beyond = pl.ds(begin + TILE, TILE)
        ey_up = rotate(pair_of(from_up.at[0], 0, where), end_cos, end_sin)
        ez_up = rotate(pair_of(from_up.at[0], 2, where), end_cos, end_sin)
        for part in range(2):
            h_yz(part, last, begin, ey_up[part], ez_up[part])
        copy_ghost(chunk).start()
        for part in range(2):
            e_yz(
                part, last, begin, hf[2 + part, last - 1, beyond, :], hf[4 + part, last - 1, beyond, :]
            )
        copy_up(1, chunk).start()
        between(1, last - 1, chunk, tiles, h_row)
    for chunk in range(tiles):
        copy_ghost(chunk).wait()
        begin = chunk * TILE
        beyond = pl.ds(begin + TILE, TILE)
        for part in (0, 2):
            real, imag = rotate(pair_of(ghost_h, part, beyond), start_cos, start_sin)
            ghost_h[part, beyond, :] = real
            ghost_h[part + 1, beyond, :] = imag
        for part in range(2):
            e_yz(part, 0, begin, ghost_h[part, beyond, :], ghost_h[2 + part, beyond, :])
        copy_down(1, chunk).start()
    finish_ghost()

    def advance(step, carry):
        slot = lax.rem(step, 2)
        drive = waveform[step - 1]
        finish_electric(drive)

        @pl.when(step == INTERVAL)
        def _():
            for x in (0, 1, last - 1, last):
                add_power(0, x)

        begin_magnetic()
        greet(step)
        for chunk in range(tiles):

            if chunk == 0:

                @pl.when(step > 1)
                def _():
                    pl.semaphore_wait(pace, 1)
            receive(slot, chunk)
            copy_up(1 - slot, chunk).start()
            copy_down(1 - slot, chunk).start()

            if chunk == tiles - 1:

                @pl.when(step < steps - 2)
                def _():
                    pl.semaphore_signal(pace, inc=1, device_id=(core_peer, sp), device_id_type=MESH)
            if chunk < half:
                between(2, last - 1, chunk, half, functools.partial(e_row, drive))
            else:
                between(1, last - 1, chunk - half, tiles - half, h_row)

        @pl.when(step == INTERVAL)
        def _():
            def add(x, inner):
                add_power(0, x)
                return inner

            lax.fori_loop(2, last - 1, add, 0)

        return carry

    lax.fori_loop(1, steps - 1, advance, 0)

    slot = (steps - 1) % 2
    drive = waveform[steps - 2]
    finish_electric(drive)
    lax.fori_loop(2, last - 1, functools.partial(e_row, drive), 0)
    begin_magnetic()
    lax.fori_loop(1, last - 1, h_row_out, 0)
    for x in (0, last - 1):
        for part in range(6):
            h_out[0, part, x] = hf[part, x, inside, :]
    final = waveform[steps - 1]
    lax.fori_loop(1, last, functools.partial(e_row_out, final), 0)
    e_x_plane(0, final)
    for chunk in range(tiles):
        receive(slot, chunk)
    fill_h_edge(last, (4,))
    e_x_plane(last, final)
    add_power(NSNAP - 1, 0)
    add_power(NSNAP - 1, last)

    at_row = lax.broadcasted_iota(jnp.int32, (1, depth), 1)
    mine = jnp.zeros((1, depth), F32)
    for snap in range(NSNAP):
        power = jnp.sum(totals[snap], axis=0, keepdims=True)
        moved = pltpu.roll(power, depth - (PML + 6) + snap, 1)
        mine = jnp.where(at_row == snap, moved, mine)
    plane_sums[0] = mine

    group = points // heights
    place = lax.rem(ka, group)

    def plane_copy(index):
        offset = lax.rem(index + plane // 2, plane - 1) + 1
        peer = ka - place + lax.rem(place + offset // slabs, group)
        return pltpu.make_async_remote_copy(
            src_ref=plane_sums.at[0],
            dst_ref=plane_sums.at[offset],
            send_sem=plane_send,
            recv_sem=plane_recv,
            device_id=(peer, lax.rem(sp + lax.rem(offset, slabs), slabs)),
            device_id_type=MESH,
        )

    def height_copy(index):
        offset = lax.rem(index + heights // 2 - 1, heights - 1) + 1
        return pltpu.make_async_remote_copy(
            src_ref=height_sums.at[0],
            dst_ref=height_sums.at[offset],
            send_sem=height_send,
            recv_sem=height_recv,
            device_id=(lax.rem(ka + group * offset, points), sp),
            device_id_type=MESH,
        )

    def started(copy):
        def start(index, carry):
            copy(index).start()
            return carry

        return start

    def wait_all(sums, count, semaphore):
        others = sums.at[pl.ds(1, count - 1)]
        pltpu.make_async_copy(others, others, semaphore).wait()

    lax.fori_loop(0, plane - 1, started(plane_copy), 0)
    for x in (0, last):
        for part in range(6):
            e_out[0, part, x] = ef[part, x, whole, :]
    for part in range(6):
        h_out[0, part, last] = hf[part, last, inside, :]
    wait_all(plane_sums, plane, plane_recv)
    slab_total = plane_sums[0]
    for offset in range(1, slabs):
        slab_total = slab_total + plane_sums[offset]
    total = slab_total
    for offset in range(slabs, plane):
        total = total + plane_sums[offset]
    height_sums[0] = total
    lax.fori_loop(0, heights - 1, started(height_copy), 0)
    cells = rows * slabs * width
    sums_out[pl.ds(0, 1), :] = slab_total / cells
    wait_all(plane_sums, plane, plane_send)
    wait_all(height_sums, heights, height_recv)
    total = height_sums[0]
    for offset in range(1, heights):
        total = total + height_sums[offset]
    sums_out[pl.ds(1, 1), :] = total / cells / points
    wait_all(height_sums, heights, height_send)


def in_hbm(values):
    return pltpu.with_memory_space_constraint(values, pltpu.HBM)


def on_device(
    bloch_index,
    material,
    permittivity,
    absorption_peak,
    source_sheet,
    waveform,
    electric_in,
    magnetic_in,
):
    rows, width, depth = material.shape
    slabs = lax.axis_size("sp")
    points = lax.axis_size("ka")
    tiles = width // TILE
    vmem = pl.BlockSpec(memory_space=pltpu.VMEM)
    hbm = pl.BlockSpec(memory_space=pltpu.HBM)
    dma = pltpu.SemaphoreType.DMA
    electric_out, magnetic_out, sums = pl.pallas_call(
        functools.partial(kernel, (points, slabs, rows, width, depth)),
        out_shape=(
            jax.ShapeDtypeStruct(electric_in.shape, F32),
            jax.ShapeDtypeStruct(magnetic_in.shape, F32),
            jax.ShapeDtypeStruct((2, depth), F32),
        ),
        in_specs=[hbm, hbm, pl.BlockSpec(memory_space=pltpu.SMEM)] + [hbm] * 5,
        out_specs=(vmem, vmem, vmem),
        scratch_shapes=[
            pltpu.SMEM(bloch_index.shape, jnp.int32),
            pltpu.SMEM(permittivity.shape, F32),
            pltpu.SMEM(waveform.shape, F32),
            pltpu.VMEM((6, rows, width + TILE, depth), F32),
            pltpu.VMEM((6, rows, width + TILE, depth), F32),
            pltpu.VMEM((6, rows, width, depth), jnp.bfloat16),
            pltpu.VMEM((6, rows, width, depth), jnp.bfloat16),
            pltpu.VMEM((rows, width, depth), jnp.int32),
            pltpu.VMEM((rows, width, depth), F32),
            pltpu.VMEM((rows, width, depth), F32),
            pltpu.VMEM((2, rows, width), F32),
            pltpu.VMEM((2, rows, width, depth), F32),
            pltpu.VMEM((2, 4, width, depth), F32),
            pltpu.VMEM((2, 4, width, depth), F32),
            pltpu.VMEM((4, width + TILE, depth), F32),
            pltpu.VMEM((2, width + TILE, depth), F32),
            pltpu.VMEM((width, depth), F32),
            pltpu.VMEM((2, TILE, width), F32),
            pltpu.VMEM((width, depth), F32),
            pltpu.VMEM((width, depth), F32),
            pltpu.VMEM((2, width, depth), F32),
            pltpu.VMEM((width, depth), F32),
            pltpu.VMEM((NSNAP, TILE, depth), F32),
            pltpu.VMEM((4 * slabs, 1, depth), F32),
            pltpu.VMEM((points // 4, 1, depth), F32),
            dma((11,)),
            dma((tiles,)),
            dma((2, tiles)),
            dma((tiles,)),
            dma((2, tiles)),
            dma((tiles,)),
            dma((tiles,)),
            dma((3,)),
            dma((3,)),
            dma,
            dma,
            dma,
            dma,
            pltpu.SemaphoreType.REGULAR((6,)),
            pltpu.SemaphoreType.REGULAR,
        ],
        compiler_params=pltpu.CompilerParams(
            collective_id=0, has_side_effects=True, vmem_limit_bytes=32 * 2**20
        ),
        name="yee",
    )(
        in_hbm(bloch_index),
        in_hbm(permittivity),
        absorption_peak,
        in_hbm(waveform),
        in_hbm(source_sheet),
        in_hbm(material),
        in_hbm(electric_in),
        in_hbm(magnetic_in),
    )
    return (electric_out, magnetic_out, sums[:1, :NSNAP], sums[1, :NSNAP])


def solution(mesh):
    in_specs = (
        P("ka", None),
        P("sp", None, None),
        P(),
        P(),
        P("ka", None, "sp", None),
        P(),
        P("ka", None, "sp", None, None),
        P("ka", None, "sp", None, None),
    )
    out_specs = (
        P("ka", None, "sp", None, None),
        P("ka", None, "sp", None, None),
        P("ka", None),
        P(),
    )
    return jax.shard_map(
        on_device, mesh=mesh, in_specs=in_specs, out_specs=out_specs, check_vma=False
    )
```

```python
import functools

import jax
import jax.numpy as jnp
from jax import lax
from jax.experimental import pallas as pl
from jax.experimental.pallas import tpu as pltpu
from jax.sharding import PartitionSpec as P

PML = 16
INTERVAL = 5
NSNAP = 2
MPHASE = 64
NMAT = 3
TIME_STEP = 0.5

MESH = pl.DeviceIdType.MESH
F32 = jnp.float32
TILE = 8


def kernel(
    sizes,
    bloch_in,
    permittivity_in,
    absorption_peak,
    waveform_in,
    sheet_in,
    material,
    e_in,
    h_in,
    e_out,
    h_out,
    sums_out,
    bloch,
    permittivity,
    waveform,
    ef,
    hf,
    e_low,
    h_low,
    mat,
    keep,
    gain,
    sheet_raw,
    sheet,
    from_up,
    from_down,
    ghost_h,
    ghost_ex,
    ghost_kind,
    ghost_raw,
    ghost_keep,
    ghost_gain,
    ghost_sheet,
    my_kind,
    totals,
    plane_sums,
    height_sums,
    load_sem,
    up_send,
    up_recv,
    down_send,
    down_recv,
    ghost_send,
    ghost_recv,
    extra_send,
    extra_recv,
    plane_send,
    plane_recv,
    height_send,
    height_recv,
    hello,
    pace,
):
    points, slabs, rows, width, depth = sizes
    ka = lax.axis_index("ka")
    sp = lax.axis_index("sp")
    up = lax.rem(sp + 1, slabs)
    down = lax.rem(sp + slabs - 1, slabs)
    tiles = width // TILE
    last = rows - 1
    steps = NSNAP * INTERVAL
    heights = points // 4
    plane = 4 * slabs
    inside = pl.ds(TILE, width)
    whole = pl.ds(0, width)

    z_above_1 = lax.rem(ka + 4, points)
    z_below_1 = lax.rem(ka + points - 4, points)
    z_above_2 = lax.rem(ka + 8, points)
    z_below_2 = lax.rem(ka + points - 8, points)
    core_peer = ka + 1 - 2 * lax.rem(ka, 2)
    x_peer = ka + 2 - 4 * lax.rem(ka // 2, 2)

    barrier = pltpu.get_barrier_semaphore()
    near = [(ka, up), (ka, down)]
    near += [(peer, sp) for peer in (z_above_1, z_below_1, core_peer, x_peer)]
    for device in near:
        pl.semaphore_signal(barrier, inc=1, device_id=device, device_id_type=MESH)

    greetings = {
        0: ((), ((0, z_above_1), (1, z_below_1))),
        1: ((0, 1), ((2, z_above_2), (3, z_below_2))),
        2: ((2, 3), ()),
        5: ((), ((4, core_peer),)),
        6: ((4,), ((5, x_peer),)),
        7: ((5,), ()),
    }

    def exchange_greetings(index):
        waits, signals = greetings[index]
        for place in waits:
            pl.semaphore_wait(hello.at[place], 1)
        for place, peer in signals:
            pl.semaphore_signal(
                hello.at[place], inc=1, device_id=(peer, sp), device_id_type=MESH
            )

    def greet(step):
        for index in greetings:
            if index > 0:
                pl.when(step == index)(functools.partial(exchange_greetings, index))

    def load(source, target, index):
        copy = pltpu.make_async_copy(source, target, load_sem.at[index])
        copy.start()
        return copy

    middle = pl.ds(1, rows - 2)
    load_first = load(e_in.at[0, :, 0], e_low.at[:, 0], 0)
    load_last = load(e_in.at[0, :, last], e_low.at[:, last], 1)
    load_h_last = load(h_in.at[0, :, last], h_low.at[:, last], 2)
    load_mat_last = load(material.at[last], mat.at[last], 3)
    load_sheet = load(sheet_in.at[0], sheet_raw, 4)
    load_e = load(e_in.at[0, :, middle], e_low.at[:, middle], 5)
    load_h = load(h_in.at[0, :, pl.ds(0, last)], h_low.at[:, pl.ds(0, last)], 6)
    load_mat = load(material.at[pl.ds(0, last)], mat.at[pl.ds(0, last)], 7)
    small = [
        load(bloch_in, bloch, 8),
        load(permittivity_in, permittivity, 9),
        load(waveform_in, waveform, 10),
    ]

    def remote(source, target, send, recv, other):
        return pltpu.make_async_remote_copy(
            src_ref=source,
            dst_ref=target,
            send_sem=send,
            recv_sem=recv,
            device_id=(ka, other),
            device_id_type=MESH,
        )

    def copy_up(slot, chunk):
        where = pl.ds(chunk * TILE, TILE)
        return remote(
            ef.at[pl.ds(2, 4), last, where],
            from_down.at[slot, :, where],
            up_send.at[chunk],
            up_recv.at[slot, chunk],
            up,
        )

    def copy_down(slot, chunk):
        where = pl.ds(chunk * TILE, TILE)
        return remote(
            ef.at[pl.ds(2, 4), 0, where],
            from_up.at[slot, :, where],
            down_send.at[chunk],
            down_recv.at[slot, chunk],
            down,
        )

    def copy_ghost(chunk):
        where = pl.ds((chunk + 1) * TILE, TILE)
        return remote(
            hf.at[pl.ds(2, 4), last, where],
            ghost_h.at[:, where],
            ghost_send.at[chunk],
            ghost_recv.at[chunk],
            up,
        )

    extras = [
        remote(
            ef.at[pl.ds(0, 2), last, whole],
            ghost_ex.at[:, whole],
            extra_send.at[0],
            extra_recv.at[0],
            up,
        ),
        remote(my_kind, ghost_kind, extra_send.at[1], extra_recv.at[1], up),
        remote(
            sheet_raw.at[:, pl.ds(rows - TILE, TILE)],
            ghost_raw,
            extra_send.at[2],
            extra_recv.at[2],
            up,
        ),
    ]

    load_first.wait()
    for part in range(2, 6):
        ef[part, 0, whole, :] = e_low[part, 0].astype(F32)
    pl.semaphore_wait(barrier, len(near))
    for chunk in range(tiles):
        copy_down(0, chunk).start()
    load_last.wait()
    for part in range(6):
        ef[part, last, whole, :] = e_low[part, last].astype(F32)
    extras[0].start()
    load_mat_last.wait()
    my_kind[...] = mat[last].astype(F32)
    extras[1].start()
    load_sheet.wait()
    extras[2].start()
    load_h_last.wait()
    for part in range(6):
        hf[part, last, inside, :] = h_low[part, last].astype(F32)
    for part in range(2):
        ef[part, 0, whole, :] = e_low[part, 0].astype(F32)
    for copy in small:
        copy.wait()

    angle_x = jnp.full((1, depth), 2.0 * jnp.pi * bloch[0, 0].astype(F32) / MPHASE, F32)
    angle_y = jnp.full((1, depth), 2.0 * jnp.pi * bloch[0, 1].astype(F32) / MPHASE, F32)
    cos_x, sin_x = jnp.cos(angle_x), jnp.sin(angle_x)
    cos_y, sin_y = jnp.cos(angle_y), jnp.sin(angle_y)
    at_end = sp == slabs - 1
    at_start = sp == 0
    end_cos = jnp.where(at_end, cos_x, 1.0)
    end_sin = jnp.where(at_end, sin_x, 0.0)
    start_cos = jnp.where(at_start, cos_x, 1.0)
    start_sin = jnp.where(at_start, -sin_x, 0.0)

    lane = lax.broadcasted_iota(jnp.int32, (TILE, depth), 1)
    at_top = lane == depth - 1
    at_bottom = lane == 0

    def z_above(values):
        return jnp.where(at_top, 0.0, pltpu.roll(values, depth - 1, 1))

    def z_below(values):
        return jnp.where(at_bottom, 0.0, pltpu.roll(values, 1, 1))

    height = lane.astype(F32)
    low_depth = jnp.maximum(PML - height, 0.0) / PML
    high_depth = jnp.maximum(height - (depth - 1 - PML), 0.0) / PML
    conduct = absorption_peak[0] * (low_depth**3 + high_depth**3)
    half_mag = conduct * (0.5 * TIME_STEP)
    h_keep = (1.0 - half_mag) / (1.0 + half_mag)
    h_gain = -TIME_STEP / (1.0 + half_mag)

    def rotate(pair, cosine, sine):
        return (pair[0] * cosine - pair[1] * sine, pair[0] * sine + pair[1] * cosine)

    def upper_edge(refs):
        first, edge = pl.ds(0, 1), pl.ds(width, 1)
        real, imag = rotate((refs[0][first, :], refs[1][first, :]), cos_y, sin_y)
        refs[0][edge, :] = real
        refs[1][edge, :] = imag

    def lower_edge(refs):
        end, edge = pl.ds(width + TILE - 1, 1), pl.ds(TILE - 1, 1)
        real, imag = rotate((refs[0][end, :], refs[1][end, :]), cos_y, -sin_y)
        refs[0][edge, :] = real
        refs[1][edge, :] = imag

    def fill_e_edge(x):
        for part in (0, 4):
            upper_edge((ef.at[part, x], ef.at[part + 1, x]))

    def fill_h_edge(x, parts=(0, 4)):
        for part in parts:
            lower_edge((hf.at[part, x], hf.at[part + 1, x]))

    def fill_ghost_ex_edge():
        upper_edge((ghost_ex.at[0], ghost_ex.at[1]))

    def fill_ghost_h_edge():
        lower_edge((ghost_h.at[2], ghost_h.at[3]))

    keeps = []
    gains = []
    for level in range(NMAT):
        relative = jnp.full((TILE, depth), permittivity[level], F32)
        half_ele = conduct * (0.5 * TIME_STEP) / relative
        keeps.append((1.0 - half_ele) / (1.0 + half_ele))
        gains.append(TIME_STEP / relative / (1.0 + half_ele))

    def choose(kind, table, zero, one):
        return jnp.where(kind == zero, table[0], jnp.where(kind == one, table[1], table[2]))

    load_e.wait()
    load_h.wait()
    load_mat.wait()

    def widen_e(x, carry):
        for part in range(6):
            ef[part, x, whole, :] = e_low[part, x].astype(F32)
        fill_e_edge(x)
        return carry

    def widen_h(x, carry):
        for part in range(6):
            hf[part, x, inside, :] = h_low[part, x].astype(F32)
        return carry

    def fill_coefficients(x, carry):
        for tile in range(tiles):
            where = pl.ds(tile * TILE, TILE)
            kind = mat[x, where, :]
            keep[x, where, :] = choose(kind, keeps, 0, 1)
            gain[x, where, :] = choose(kind, gains, 0, 1)
        return carry

    fill_e_edge(0)
    fill_e_edge(last)
    lax.fori_loop(1, last, widen_e, 0)
    lax.fori_loop(0, last, widen_h, 0)
    lax.fori_loop(0, rows, fill_coefficients, 0)

    at_sheet = lax.broadcasted_iota(jnp.int32, (width, depth), 1) == PML + 2
    for part in range(2):
        turned = sheet_raw[part].T
        for x in range(rows):
            spread = jnp.broadcast_to(turned[:, x : x + 1], (width, depth))
            sheet[part, x] = jnp.where(at_sheet, spread, 0.0)

    def h_x(part, x, begin):
        ey = ef[2 + part, x, pl.ds(begin, TILE), :]
        ez = ef[4 + part, x, pl.ds(begin, TILE), :]
        ez_y = ef[4 + part, x, pl.ds(begin + 1, TILE), :]
        change = (ez_y - ez) - (z_above(ey) - ey)
        where = pl.ds(begin + TILE, TILE)
        hf[part, x, where, :] = h_keep * hf[part, x, where, :] + h_gain * change

    def h_yz(part, x, begin, ey_x, ez_x):
        ex = ef[part, x, pl.ds(begin, TILE), :]
        ex_y = ef[part, x, pl.ds(begin + 1, TILE), :]
        ey = ef[2 + part, x, pl.ds(begin, TILE), :]
        ez = ef[4 + part, x, pl.ds(begin, TILE), :]
        where = pl.ds(begin + TILE, TILE)
        change_y = (z_above(ex) - ex) - (ez_x - ez)
        change_z = (ey_x - ey) - (ex_y - ex)
        hf[2 + part, x, where, :] = h_keep * hf[2 + part, x, where, :] + h_gain * change_y
        hf[4 + part, x, where, :] = h_keep * hf[4 + part, x, where, :] + h_gain * change_z

    def ghost_h_yz(part, begin, ey, ez):
        ex = ghost_ex[part, pl.ds(begin, TILE), :]
        ex_y = ghost_ex[part, pl.ds(begin + 1, TILE), :]
        ey_x = ef[2 + part, 0, pl.ds(begin, TILE), :]
        ez_x = ef[4 + part, 0, pl.ds(begin, TILE), :]
        where = pl.ds(begin + TILE, TILE)
        change_y = (z_above(ex) - ex) - (ez_x - ez)
        change_z = (ey_x - ey) - (ex_y - ex)
        ghost_h[part, where, :] = h_keep * ghost_h[part, where, :] + h_gain * change_y
        ghost_h[2 + part, where, :] = h_keep * ghost_h[2 + part, where, :] + h_gain * change_z

    def e_x(part, x, begin, drive):
        where = pl.ds(begin, TILE)
        hy = hf[2 + part, x, pl.ds(begin + TILE, TILE), :]
        hz = hf[4 + part, x, pl.ds(begin + TILE, TILE), :]
        hz_y = hf[4 + part, x, pl.ds(begin + TILE - 1, TILE), :]
        change = (hz - hz_y) - (hy - z_below(hy)) - drive * sheet[part, x, where, :]
        ef[part, x, where, :] = (
            keep[x, where, :] * ef[part, x, where, :] + gain[x, where, :] * change
        )

    def ghost_e_x(part, begin, drive):
        where = pl.ds(begin, TILE)
        hy = ghost_h[part, pl.ds(begin + TILE, TILE), :]
        hz = ghost_h[2 + part, pl.ds(begin + TILE, TILE), :]
        hz_y = ghost_h[2 + part, pl.ds(begin + TILE - 1, TILE), :]
        change = (hz - hz_y) - (hy - z_below(hy)) - drive * ghost_sheet[part, where, :]
        ghost_ex[part, where, :] = (
            ghost_keep[where, :] * ghost_ex[part, where, :] + ghost_gain[where, :] * change
        )

    def e_yz(part, x, begin, hy_x, hz_x):
        where = pl.ds(begin, TILE)
        hx = hf[part, x, pl.ds(begin + TILE, TILE), :]
        hx_y = hf[part, x, pl.ds(begin + TILE - 1, TILE), :]
        hy = hf[2 + part, x, pl.ds(begin + TILE, TILE), :]
        hz = hf[4 + part, x, pl.ds(begin + TILE, TILE), :]
        change_y = (hx - z_below(hx)) - (hz - hz_x)
        change_z = (hy - hy_x) - (hx - hx_y)
        retain = keep[x, where, :]
        factor = gain[x, where, :]
        ef[2 + part, x, where, :] = retain * ef[2 + part, x, where, :] + factor * change_y
        ef[4 + part, x, where, :] = retain * ef[4 + part, x, where, :] + factor * change_z

    def h_row(x, carry):
        for tile in range(tiles):
            begin = tile * TILE
            where = pl.ds(begin, TILE)
            for part in range(2):
                h_x(part, x, begin)
                h_yz(
                    part, x, begin, ef[2 + part, x + 1, where, :], ef[4 + part, x + 1, where, :]
                )
        fill_h_edge(x)
        return carry

    def h_row_out(x, carry):
        h_row(x, carry)
        for part in range(6):
            h_out[0, part, x] = hf[part, x, inside, :]
        return carry

    def e_row(drive, x, carry):
        for tile in range(tiles):
            begin = tile * TILE
            where = pl.ds(begin + TILE, TILE)
            for part in range(2):
                e_x(part, x, begin, drive)
                e_yz(
                    part, x, begin, hf[2 + part, x - 1, where, :], hf[4 + part, x - 1, where, :]
                )
        fill_e_edge(x)
        return carry

    def add_power(index, x, parts=(0, 1, 2, 3), chosen=range(tiles)):
        total = totals[index]
        for part in parts:
            for tile in chosen:
                values = ef[part, x, pl.ds(tile * TILE, TILE), :]
                total = total + values * values
        totals[index] = total

    def e_row_out(drive, x, carry):
        e_row(drive, x, carry)
        for part in range(6):
            e_out[0, part, x] = ef[part, x, whole, :]
        add_power(NSNAP - 1, x)
        return carry

    def e_x_plane(x, drive):
        for tile in range(tiles):
            for part in range(2):
                e_x(part, x, tile * TILE, drive)

    def finish_electric(drive):
        fill_h_edge(last, (4,))
        fill_ghost_h_edge()
        for tile in range(tiles):
            for part in range(2):
                ghost_e_x(part, tile * TILE, drive)
        fill_ghost_ex_edge()
        e_x_plane(0, drive)
        e_x_plane(last, drive)
        fill_e_edge(0)
        fill_e_edge(last)
        e_row(drive, 1, 0)
        e_row(drive, last - 1, 0)

    def begin_magnetic():
        h_row(0, 0)
        h_row(last - 1, 0)
        for tile in range(tiles):
            for part in range(2):
                h_x(part, last, tile * TILE)
        fill_h_edge(last, (0,))

    def pair_of(ref, part, where):
        return (ref[part, where, :], ref[part + 1, where, :])

    def receive(slot, chunk):
        arriving_up = copy_up(slot, chunk)
        arriving_down = copy_down(slot, chunk)
        arriving_up.wait()
        arriving_down.wait()
        begin = chunk * TILE
        where = pl.ds(begin, TILE)
        ey_up = rotate(pair_of(from_up.at[slot], 0, where), end_cos, end_sin)
        ez_up = rotate(pair_of(from_up.at[slot], 2, where), end_cos, end_sin)
        ey_down = rotate(pair_of(from_down.at[slot], 0, where), start_cos, start_sin)
        ez_down = rotate(pair_of(from_down.at[slot], 2, where), start_cos, start_sin)
        beyond = pl.ds(begin + TILE, TILE)
        for part in range(2):
            h_yz(part, last, begin, ey_up[part], ez_up[part])
            ghost_h_yz(part, begin, ey_down[part], ez_down[part])
        for part in range(2):
            e_yz(part, last, begin, hf[2 + part, last - 1, beyond, :], hf[4 + part, last - 1, beyond, :])
            e_yz(part, 0, begin, ghost_h[part, beyond, :], ghost_h[2 + part, beyond, :])

    def share(first, end, part, pieces):
        count = end - first
        return first + count * part // pieces, first + count * (part + 1) // pieces

    totals[...] = jnp.zeros(totals.shape, F32)

    def finish_ghost():
        for extra in extras:
            extra.wait()
        real, imag = rotate((ghost_ex[0, whole, :], ghost_ex[1, whole, :]), start_cos, start_sin)
        ghost_ex[0, whole, :] = real
        ghost_ex[1, whole, :] = imag
        for tile in range(tiles):
            where = pl.ds(tile * TILE, TILE)
            kind = ghost_kind[where, :]
            ghost_keep[where, :] = choose(kind, keeps, 0.0, 1.0)
            ghost_gain[where, :] = choose(kind, gains, 0.0, 1.0)
        real, imag = rotate(
            (ghost_raw[0], ghost_raw[1]), start_cos[:, :width], start_sin[:, :width]
        )
        for part, raw in enumerate((real, imag)):
            column = raw.T[:, TILE - 1 : TILE]
            spread = jnp.broadcast_to(column, (width, depth))
            ghost_sheet[part] = jnp.where(at_sheet, spread, 0.0)

    half = tiles // 2

    def between(first, end, part, pieces, row):
        begin, end = share(first, end, part, pieces)
        lax.fori_loop(begin, end, row, 0)

    begin_magnetic()
    exchange_greetings(0)
    for chunk in range(tiles):
        copy_down(0, chunk).wait()
        begin = chunk * TILE
        where = pl.ds(begin, TILE)
        beyond = pl.ds(begin + TILE, TILE)
        ey_up = rotate(pair_of(from_up.at[0], 0, where), end_cos, end_sin)
        ez_up = rotate(pair_of(from_up.at[0], 2, where), end_cos, end_sin)
        for part in range(2):
            h_yz(part, last, begin, ey_up[part], ez_up[part])
        copy_ghost(chunk).start()
        for part in range(2):
            e_yz(
                part, last, begin, hf[2 + part, last - 1, beyond, :], hf[4 + part, last - 1, beyond, :]
            )
        copy_up(1, chunk).start()
        between(1, last - 1, chunk, tiles, h_row)
    for chunk in range(tiles):
        copy_ghost(chunk).wait()
        begin = chunk * TILE
        beyond = pl.ds(begin + TILE, TILE)
        for part in (0, 2):
            real, imag = rotate(pair_of(ghost_h, part, beyond), start_cos, start_sin)
            ghost_h[part, beyond, :] = real
            ghost_h[part + 1, beyond, :] = imag
        for part in range(2):
            e_yz(part, 0, begin, ghost_h[part, beyond, :], ghost_h[2 + part, beyond, :])
        copy_down(1, chunk).start()
    finish_ghost()

    def advance(step, carry):
        slot = lax.rem(step, 2)
        drive = waveform[step - 1]
        finish_electric(drive)

        @pl.when(step == INTERVAL)
        def _():
            for x in (0, 1, last - 1, last):
                add_power(0, x)

        begin_magnetic()
        greet(step)
        for chunk in range(tiles):

            if chunk == 0:

                @pl.when(step > 1)
                def _():
                    pl.semaphore_wait(pace, 1)
            receive(slot, chunk)
            copy_up(1 - slot, chunk).start()
            copy_down(1 - slot, chunk).start()

            if chunk == tiles - 1:

                @pl.when(step < steps - 2)
                def _():
                    pl.semaphore_signal(pace, inc=1, device_id=(core_peer, sp), device_id_type=MESH)
            if chunk < half:
                between(2, last - 1, chunk, half, functools.partial(e_row, drive))
            else:
                between(1, last - 1, chunk - half, tiles - half, h_row)

        @pl.when(step == INTERVAL)
        def _():
            def add(x, inner):
                add_power(0, x)
                return inner

            lax.fori_loop(2, last - 1, add, 0)

        return carry

    lax.fori_loop(1, steps - 1, advance, 0)

    slot = (steps - 1) % 2
    drive = waveform[steps - 2]
    finish_electric(drive)
    lax.fori_loop(2, last - 1, functools.partial(e_row, drive), 0)
    begin_magnetic()
    lax.fori_loop(1, last - 1, h_row_out, 0)
    for x in (0, last - 1):
        for part in range(6):
            h_out[0, part, x] = hf[part, x, inside, :]
    final = waveform[steps - 1]
    lax.fori_loop(1, last, functools.partial(e_row_out, final), 0)
    e_x_plane(0, final)
    add_power(NSNAP - 1, 0, (0, 1))
    for chunk in range(tiles):
        receive(slot, chunk)
        for x in (0, last):
            add_power(NSNAP - 1, x, (2, 3), (chunk,))
    fill_h_edge(last, (4,))
    e_x_plane(last, final)
    add_power(NSNAP - 1, last, (0, 1))

    at_row = lax.broadcasted_iota(jnp.int32, (1, depth), 1)
    mine = jnp.zeros((1, depth), F32)
    for snap in range(NSNAP):
        power = jnp.sum(totals[snap], axis=0, keepdims=True)
        moved = pltpu.roll(power, depth - (PML + 6) + snap, 1)
        mine = jnp.where(at_row == snap, moved, mine)
    plane_sums[0] = mine

    group = points // heights
    place = lax.rem(ka, group)

    def plane_copy(index):
        offset = (index + plane // 2) % (plane - 1) + 1
        peer = ka - place + lax.rem(place + offset // slabs, group)
        return pltpu.make_async_remote_copy(
            src_ref=plane_sums.at[0],
            dst_ref=plane_sums.at[offset],
            send_sem=plane_send,
            recv_sem=plane_recv,
            device_id=(peer, lax.rem(sp + offset % slabs, slabs)),
            device_id_type=MESH,
        )

    def height_copy(index):
        offset = (index + heights // 2 - 1) % (heights - 1) + 1
        return pltpu.make_async_remote_copy(
            src_ref=height_sums.at[0],
            dst_ref=height_sums.at[offset],
            send_sem=height_send,
            recv_sem=height_recv,
            device_id=(lax.rem(ka + group * offset, points), sp),
            device_id_type=MESH,
        )

    def wait_all(sums, count, semaphore):
        others = sums.at[pl.ds(1, count - 1)]
        pltpu.make_async_copy(others, others, semaphore).wait()

    for index in range(plane - 1):
        plane_copy(index).start()
    for x in (0, last):
        for part in range(6):
            e_out[0, part, x] = ef[part, x, whole, :]
    for part in range(6):
        h_out[0, part, last] = hf[part, last, inside, :]
    wait_all(plane_sums, plane, plane_recv)
    slab_total = plane_sums[0]
    for offset in range(1, slabs):
        slab_total = slab_total + plane_sums[offset]
    total = slab_total
    for offset in range(slabs, plane):
        total = total + plane_sums[offset]
    height_sums[0] = total
    for index in range(heights - 1):
        height_copy(index).start()
    cells = rows * slabs * width
    sums_out[pl.ds(0, 1), :] = slab_total / cells
    wait_all(plane_sums, plane, plane_send)
    wait_all(height_sums, heights, height_recv)
    total = height_sums[0]
    for offset in range(1, heights):
        total = total + height_sums[offset]
    sums_out[pl.ds(1, 1), :] = total / cells / points
    wait_all(height_sums, heights, height_send)


def in_hbm(values):
    return pltpu.with_memory_space_constraint(values, pltpu.HBM)


def on_device(
    bloch_index,
    material,
    permittivity,
    absorption_peak,
    source_sheet,
    waveform,
    electric_in,
    magnetic_in,
):
    rows, width, depth = material.shape
    slabs = lax.axis_size("sp")
    points = lax.axis_size("ka")
    tiles = width // TILE
    vmem = pl.BlockSpec(memory_space=pltpu.VMEM)
    hbm = pl.BlockSpec(memory_space=pltpu.HBM)
    dma = pltpu.SemaphoreType.DMA
    electric_out, magnetic_out, sums = pl.pallas_call(
        functools.partial(kernel, (points, slabs, rows, width, depth)),
        out_shape=(
            jax.ShapeDtypeStruct(electric_in.shape, F32),
            jax.ShapeDtypeStruct(magnetic_in.shape, F32),
            jax.ShapeDtypeStruct((2, depth), F32),
        ),
        in_specs=[hbm, hbm, pl.BlockSpec(memory_space=pltpu.SMEM)] + [hbm] * 5,
        out_specs=(vmem, vmem, vmem),
        scratch_shapes=[
            pltpu.SMEM(bloch_index.shape, jnp.int32),
            pltpu.SMEM(permittivity.shape, F32),
            pltpu.SMEM(waveform.shape, F32),
            pltpu.VMEM((6, rows, width + TILE, depth), F32),
            pltpu.VMEM((6, rows, width + TILE, depth), F32),
            pltpu.VMEM((6, rows, width, depth), jnp.bfloat16),
            pltpu.VMEM((6, rows, width, depth), jnp.bfloat16),
            pltpu.VMEM((rows, width, depth), jnp.int32),
            pltpu.VMEM((rows, width, depth), F32),
            pltpu.VMEM((rows, width, depth), F32),
            pltpu.VMEM((2, rows, width), F32),
            pltpu.VMEM((2, rows, width, depth), F32),
            pltpu.VMEM((2, 4, width, depth), F32),
            pltpu.VMEM((2, 4, width, depth), F32),
            pltpu.VMEM((4, width + TILE, depth), F32),
            pltpu.VMEM((2, width + TILE, depth), F32),
            pltpu.VMEM((width, depth), F32),
            pltpu.VMEM((2, TILE, width), F32),
            pltpu.VMEM((width, depth), F32),
            pltpu.VMEM((width, depth), F32),
            pltpu.VMEM((2, width, depth), F32),
            pltpu.VMEM((width, depth), F32),
            pltpu.VMEM((NSNAP, TILE, depth), F32),
            pltpu.VMEM((4 * slabs, 1, depth), F32),
            pltpu.VMEM((points // 4, 1, depth), F32),
            dma((11,)),
            dma((tiles,)),
            dma((2, tiles)),
            dma((tiles,)),
            dma((2, tiles)),
            dma((tiles,)),
            dma((tiles,)),
            dma((3,)),
            dma((3,)),
            dma,
            dma,
            dma,
            dma,
            pltpu.SemaphoreType.REGULAR((6,)),
            pltpu.SemaphoreType.REGULAR,
        ],
        compiler_params=pltpu.CompilerParams(
            collective_id=0, has_side_effects=True, vmem_limit_bytes=32 * 2**20
        ),
        name="yee",
    )(
        in_hbm(bloch_index),
        in_hbm(permittivity),
        absorption_peak,
        in_hbm(waveform),
        in_hbm(source_sheet),
        in_hbm(material),
        in_hbm(electric_in),
        in_hbm(magnetic_in),
    )
    return (electric_out, magnetic_out, sums[:1, :NSNAP], sums[1, :NSNAP])


def solution(mesh):
    in_specs = (
        P("ka", None),
        P("sp", None, None),
        P(),
        P(),
        P("ka", None, "sp", None),
        P(),
        P("ka", None, "sp", None, None),
        P("ka", None, "sp", None, None),
    )
    out_specs = (
        P("ka", None, "sp", None, None),
        P("ka", None, "sp", None, None),
        P("ka", None),
        P(),
    )
    return jax.shard_map(
        on_device, mesh=mesh, in_specs=in_specs, out_specs=out_specs, check_vma=False
    )
```
